32 devices in a mesh: rep: 4 (over x, core), shard: 8 (over z, y).
Axes of the slice: x: 2, y: 2, z: 4, core: 2. Of those that a mesh axis runs over, the one named last changes fastest.
Arguments:
- tokens: bfloat16 [64, 512, 768], P(None, ('rep', 'shard')), may hold values from -6 to 6
- lengths: int32 [64], replicated, may hold values from 1 to 512, 20480 in all
- seq_order: int32 [64], replicated, may hold values from 0 to 63, each once
- w_query: bfloat16 [768, 768], P('shard'), may hold values from -0.21875 to 0.21875
- w_key: bfloat16 [768, 768], P('shard'), may hold values from -0.21875 to 0.21875
- w_value: bfloat16 [768, 768], P('shard'), may hold values from -0.21875 to 0.21875
- w_out: bfloat16 [768, 768], P('shard'), may hold values from -0.875 to 0.875
- b_query: bfloat16 [768], P('shard'), may hold values from -3 to 3
- b_value: bfloat16 [768], P('shard'), may hold values from -3 to 3
- b_out: bfloat16 [768], P('shard'), may hold values from -3 to 3
- ln1_gain: bfloat16 [768], P('shard'), may hold values from 0.5 to 1.5
- ln1_bias: bfloat16 [768], P('shard'), may hold values from -3 to 3
- w_up: bfloat16 [768, 3072], P('shard'), may hold values from -0.21875 to 0.21875
- b_up: bfloat16 [3072], P('shard'), may hold values from -3 to 3
- w_down: bfloat16 [3072, 768], P('shard'), may hold values from -0.109375 to 0.109375
- b_down: bfloat16 [768], P('shard'), may hold values from -3 to 3
- ln2_gain: bfloat16 [768], P('shard'), may hold values from 0.5 to 1.5
- ln2_bias: bfloat16 [768], P('shard'), may hold values from -3 to 3
- cotangent: bfloat16 [64, 512, 768], P(('rep', 'shard')), may hold values from -6 to 6
Outputs:
- outputs: bfloat16 [64, 512, 768], P(('rep', 'shard'))
- grad_tokens: bfloat16 [64, 512, 768], P(None, ('rep', 'shard'))
- grad_w_query: float32 [768, 768], P('shard')
- grad_w_key: float32 [768, 768], P('shard')
- grad_w_value: float32 [768, 768], P('shard')
- grad_w_out: float32 [768, 768], P('shard')
- grad_b_query: float32 [768], P('shard')
- grad_b_value: float32 [768], P('shard')
- grad_b_out: float32 [768], P('shard')
- grad_ln1_gain: float32 [768], P('shard')
- grad_ln1_bias: float32 [768], P('shard')
- grad_w_up: float32 [768, 3072], P('shard')
- grad_b_up: float32 [3072], P('shard')
- grad_w_down: float32 [3072, 768], P('shard')
- grad_b_down: float32 [768], P('shard')
- grad_ln2_gain: float32 [768], P('shard')
- grad_ln2_bias: float32 [768], P('shard')
The draws below stay inside these ranges and needn't reach their ends.
Inputs may be any that keep to these rules, and one draw needn't show every extreme that they name: `lengths`: each sequence has 1 to 512 valid leading positions and some sequence has 512. `seq_order`: a permutation of the 64 sequences.
All inputs are finite; a program needn't handle non-finite values.
Results may differ from the reference program's by a relative error of at most 0.02.
Values may be sent and summed in bfloat16 or wider, within the bound.
A program may use at most 192 MiB of HBM per device.

```python
import math
import jax
import jax.numpy as jnp
import numpy as np
from jax import lax

D = 768
HEADS = 12
HD = 64
FF = 3072
SEQ_LEN = 512
NSEQ = 64


def steps_of(stream_key, shape, cuts, low, largest):
    def one(position, parts):
        steps = jax.random.uniform(jax.random.fold_in(jax.random.fold_in(stream_key, 6), position), (parts,), jnp.float32, low / len(cuts), largest / len(cuts))
        return jnp.repeat(jnp.exp(steps), shape[position] // parts).reshape((-1,) + (1,) * (len(shape) - position - 1))

    loudness = one(*cuts[0])
    for cut in cuts[1:]:
        loudness = loudness * one(*cut)
    return loudness


def split_up(count, total, bound, lean):
    portions = [(1 << 20) // math.isqrt(grade ** lean) + 1 for grade in range(2, count + 1)]
    surplus, given = total - bound - (count - 1), [1] * (count - 1)
    while surplus > 0:
        candidates = [i for i in range(count - 1) if given[i] < bound]
        whole, remaining = sum([portions[i] for i in candidates]), surplus
        for i in candidates:
            addition = min(bound - given[i], max(1, remaining * portions[i] // whole), surplus)
            given[i] = given[i] + addition
            surplus = surplus - addition
    return np.array([bound] + given)


def uneven(key, amount, total, most, slope):
    if amount == 2:
        one = jax.random.randint(key, (), max(1, total - most), min(most, total - 1) + 1)
        return jnp.stack([one, total - one])
    sizes = jnp.asarray(split_up(amount, total, most, slope), jnp.int32)
    couples = (amount - 1) // 2
    giver, receiver = sizes[1:1 + 2 * couples:2], sizes[2:2 + 2 * couples:2]
    room = jnp.minimum(giver - 1, most - receiver)
    shifted = jax.random.randint(jax.random.fold_in(key, 1), (couples,), 0, 1 << 20) % (room + 1)
    sizes = sizes.at[1:1 + 2 * couples:2].set(giver - shifted).at[2:2 + 2 * couples:2].set(receiver + shifted)
    return sizes[jax.random.permutation(jax.random.fold_in(key, 2), amount)]


def scatter_about(key, extent, spread, bound, pieces=(), kind=jnp.bfloat16):
    result = spread * jax.random.normal(key, extent, jnp.float32)
    if pieces:
        result = result * steps_of(key, extent, pieces, -0.22, 0.18)
    return jnp.clip(result, -bound, bound).astype(kind)


def setup_inputs(seed: int = 0) -> dict:
    arg_keys = jax.random.split(jax.random.key(seed), 20)
    tokens = scatter_about(arg_keys[0], (NSEQ, SEQ_LEN, D), 1.0, 6.0, ((1, 32),))
    lengths = uneven(arg_keys[1], NSEQ, NSEQ * SEQ_LEN * 5 // 8, SEQ_LEN, 1).astype(jnp.int32)
    seq_order = jax.random.permutation(arg_keys[2], NSEQ).astype(jnp.int32)
    w_query = scatter_about(arg_keys[3], (D, D), D ** -0.5, 0.21875, ((0, 8),))
    w_key = scatter_about(arg_keys[4], (D, D), D ** -0.5, 0.21875, ((0, 8),))
    w_value = scatter_about(arg_keys[5], (D, D), D ** -0.5, 0.21875, ((0, 8),))
    w_out = scatter_about(arg_keys[6], (D, D), (D // 16) ** -0.5, 0.875, ((0, 8),))
    b_query = scatter_about(arg_keys[7], (D,), 0.5, 3.0, ((0, 8),))
    b_value = scatter_about(arg_keys[8], (D,), 0.5, 3.0, ((0, 8),))
    b_out = scatter_about(arg_keys[9], (D,), 0.5, 3.0, ((0, 8),))
    ln1_gain = jnp.clip(1.0 + 0.1 * jax.random.normal(arg_keys[10], (D,), jnp.float32), 0.5, 1.5).astype(jnp.bfloat16)
    ln1_bias = scatter_about(arg_keys[11], (D,), 0.5, 3.0, ((0, 8),))
    w_up = scatter_about(arg_keys[12], (D, FF), D ** -0.5, 0.21875, ((0, 8),))
    b_up = scatter_about(arg_keys[13], (FF,), 0.5, 3.0, ((0, 8),))
    w_down = scatter_about(arg_keys[14], (FF, D), FF ** -0.5, 0.109375, ((0, 8),))
    b_down = scatter_about(arg_keys[15], (D,), 0.5, 3.0, ((0, 8),))
    ln2_gain = jnp.clip(1.0 + 0.1 * jax.random.normal(arg_keys[16], (D,), jnp.float32), 0.5, 1.5).astype(jnp.bfloat16)
    ln2_bias = scatter_about(arg_keys[17], (D,), 0.5, 3.0, ((0, 8),))
    cotangent = scatter_about(arg_keys[18], (NSEQ, SEQ_LEN, D), 1.0, 6.0, ((0, 32),))
    return {"tokens": tokens, "lengths": lengths, "seq_order": seq_order, "w_query": w_query, "w_key": w_key, "w_value": w_value, "w_out": w_out, "b_query": b_query, "b_value": b_value, "b_out": b_out, "ln1_gain": ln1_gain, "ln1_bias": ln1_bias, "w_up": w_up, "b_up": b_up, "w_down": w_down, "b_down": b_down, "ln2_gain": ln2_gain, "ln2_bias": ln2_bias, "cotangent": cotangent}


@jax.custom_vjp
def low(v):
    return lax.optimization_barrier(v.astype(jnp.bfloat16)).astype(jnp.float32)

@jax.custom_vjp
def low_back(v):
    return v

def low_keep(v):
    return (low(v), None)

def low_pass(kept, grad):
    return (grad,)

def back_keep(v):
    return (v, None)

def back_low(kept, grad):
    return (low(grad),)
low.defvjp(low_keep, low_pass)
low_back.defvjp(back_keep, back_low)

def matmul(left, right):
    return jnp.dot(left, right, precision=lax.Precision.HIGHEST, preferred_element_type=jnp.float32)

def layer_norm(values, gain, shift):
    row_mean = lax.optimization_barrier(jnp.mean(values, axis=-1, keepdims=True))
    centered = values - row_mean
    variance = lax.optimization_barrier(jnp.mean(centered * centered, axis=-1, keepdims=True))
    return centered * lax.rsqrt(variance + 1e-12) * gain + shift

def sequence_forward(params, sequence, length):
    w_query, w_key, w_value, w_out, b_query, b_value, b_out, ln1_gain, ln1_bias, w_up, b_up, w_down, b_down, ln2_gain, ln2_bias = params
    key_mask = jnp.arange(SEQ_LEN, dtype=jnp.int32) < length
    queries = low(low_back(matmul(sequence, w_query) + b_query))
    keys_low = low(low_back(matmul(sequence, w_key)))
    values_low = low(low_back(matmul(sequence, w_value) + b_value))
    query_heads = queries.reshape(SEQ_LEN, HEADS, HD)
    key_heads = keys_low.reshape(SEQ_LEN, HEADS, HD)
    value_heads = values_low.reshape(SEQ_LEN, HEADS, HD)
    scores = jnp.einsum('qhd,khd->hqk', query_heads, key_heads, precision=lax.Precision.HIGHEST) * HD ** (-0.5)
    scores = low_back(scores)
    scores = jnp.where(key_mask[None, None, :], scores, -1e+30)
    attn_probs = jax.nn.softmax(scores, axis=-1)
    context = jnp.einsum('hqk,khd->qhd', low(attn_probs), value_heads, precision=lax.Precision.HIGHEST)
    context = low(low_back(context.reshape(SEQ_LEN, HEADS * HD)))
    attn_out = low_back(matmul(context, w_out) + b_out)
    hidden1 = layer_norm(sequence + attn_out, ln1_gain, ln1_bias)
    up_proj = low_back(matmul(low(hidden1), w_up) + b_up)
    activated = low(jax.nn.gelu(up_proj, approximate=False))
    ffn_out = low_back(matmul(activated, w_down) + b_down)
    return layer_norm(hidden1 + ffn_out, ln2_gain, ln2_bias)

def reference(tokens, lengths, seq_order, w_query, w_key, w_value, w_out, b_query, b_value, b_out, ln1_gain, ln1_bias, w_up, b_up, w_down, b_down, ln2_gain, ln2_bias, cotangent):
    params = tuple((param.astype(jnp.float32) for param in (w_query, w_key, w_value, w_out, b_query, b_value, b_out, ln1_gain, ln1_bias, w_up, b_up, w_down, b_down, ln2_gain, ln2_bias)))
    owned = tokens.astype(jnp.float32)[seq_order]
    owned_len = lengths[seq_order]
    valid_rows = (jnp.arange(SEQ_LEN, dtype=jnp.int32)[None, :] < owned_len[:, None]).astype(jnp.float32)
    grad_out = cotangent.astype(jnp.float32) * valid_rows[:, :, None]
    checked_step = jax.checkpoint(sequence_forward)

    def all_sequences(params, owned):

        def scan_step(carried, packed):
            sequence, length = packed
            return (carried, checked_step(params, sequence, length))
        final_carry, results = lax.scan(scan_step, jnp.zeros((), jnp.float32), (owned, owned_len))
        return results
    results, pullback = jax.vjp(all_sequences, params, owned)
    param_grads, grad_owned = pullback(grad_out)
    grad_tokens = jnp.zeros(grad_owned.shape, grad_owned.dtype).at[seq_order].set(grad_owned)
    return (results.astype(jnp.bfloat16), grad_tokens.astype(jnp.bfloat16), param_grads[0], param_grads[1], param_grads[2], param_grads[3], param_grads[4], param_grads[5], param_grads[6], param_grads[7], param_grads[8], param_grads[9], param_grads[10], param_grads[11], param_grads[12], param_grads[13], param_grads[14])
```

```python
from functools import partial

import jax
import jax.numpy as jnp
from jax import lax
from jax.experimental import pallas as pl
from jax.experimental.pallas import tpu as pltpu
from jax.sharding import PartitionSpec as P

HEADS = 12
HEAD_DIM = 64
PAIR = 128
NEG_FILL = -1e30
EPS_NORM = 1e-12
LOG2E = 1.4426950408889634
MESH = pl.DeviceIdType.MESH


def contract_rows(left, right):
    return lax.dot_general(
        left, right, (((0,), (0,)), ((), ())), preferred_element_type=jnp.float32
    )


def contract_cols(left, right):
    return lax.dot_general(
        left, right, (((1,), (1,)), ((), ())), preferred_element_type=jnp.float32
    )


def norm_stats(resid):
    row_mean = jnp.mean(resid, axis=-1, keepdims=True)
    centered = resid - row_mean
    variance = jnp.mean(centered * centered, axis=-1, keepdims=True)
    inv_std = lax.rsqrt(variance + EPS_NORM)
    return (centered * inv_std, inv_std)


def norm_back(grad_in, normed, inv_std, gain):
    scaled = grad_in * gain
    mean_grad = jnp.mean(scaled, axis=-1, keepdims=True)
    mean_cross = jnp.mean(scaled * normed, axis=-1, keepdims=True)
    return inv_std * (scaled - mean_grad - normed * mean_cross)


def exact_gelu(values):
    return jax.nn.gelu(values, approximate=False)


def attend_forward_kernel(len_ref, q_ref, k_ref, v_ref, ctx_ref, probs_ref, *, scale):
    seq_len = q_ref.shape[0]
    valid = len_ref[pl.program_id(0)]
    key_pos = lax.broadcasted_iota(jnp.int32, (seq_len, PAIR), 0)
    fill = jnp.where(key_pos < valid, 0.0, NEG_FILL)[:, :1]
    first = lax.broadcasted_iota(jnp.int32, (seq_len, PAIR), 1) < HEAD_DIM
    queries = q_ref[...]
    keys = k_ref[...]
    values_t = v_ref[...].T
    parts = []
    for head in range(2):
        own = first if head == 0 else jnp.logical_not(first)
        head_keys = jnp.where(own, keys, jnp.zeros_like(keys))
        scores = lax.dot_general(head_keys, queries, (((1,), (1,)), ((), ())), preferred_element_type=jnp.float32)
        scaled = scores * (scale * LOG2E) + fill
        top = jnp.max(scaled, axis=0, keepdims=True)
        raised = jnp.exp2(scaled - top)
        total = jnp.sum(raised, axis=0, keepdims=True)
        probs = (raised * (1.0 / total)).astype(jnp.bfloat16)
        probs_ref[head] = probs
        parts.append(jnp.dot(values_t[head * HEAD_DIM : (head + 1) * HEAD_DIM], probs, preferred_element_type=jnp.float32))
    ctx_ref[...] = jnp.concatenate(parts, axis=0).T.astype(jnp.bfloat16)

def attend_forward(projected, lens, seq_count, seq_len, width, scale):
    pairs = width // PAIR
    grid_spec = pltpu.PrefetchScalarGridSpec(
        num_scalar_prefetch=1, grid=(seq_count, pairs),
        in_specs=[
            pl.BlockSpec((seq_len, PAIR), lambda s, h, n: (s, h)),
            pl.BlockSpec((seq_len, PAIR), lambda s, h, n: (s, pairs + h)),
            pl.BlockSpec((seq_len, PAIR), lambda s, h, n: (s, 2 * pairs + h)),
        ],
        out_specs=[
            pl.BlockSpec((seq_len, PAIR), lambda s, h, n: (s, h)),
            pl.BlockSpec((2, seq_len, seq_len), lambda s, h, n: (s * pairs + h, 0, 0)),
        ])
    return pl.pallas_call(
        partial(attend_forward_kernel, scale=scale), grid_spec=grid_spec,
        out_shape=[jax.ShapeDtypeStruct((seq_count * seq_len, width), jnp.bfloat16),
                   jax.ShapeDtypeStruct((seq_count * 2 * pairs, seq_len, seq_len), jnp.bfloat16)],
        compiler_params=pltpu.CompilerParams(dimension_semantics=("arbitrary", "arbitrary")),
        name="attend_forward",
    )(lens, projected, projected, projected)

def attend_backward_kernel(q_ref, k_ref, v_ref, gctx_ref, probs_ref, out_ref, *, scale):
    seq_len = q_ref.shape[0]
    width = out_ref.shape[1] // 3
    first = lax.broadcasted_iota(jnp.int32, (seq_len, PAIR), 1) < HEAD_DIM
    queries = q_ref[...]
    keys_t = k_ref[...].T
    values = v_ref[...]
    grad_ctx = gctx_ref[...]
    gq_parts, gk_parts, gv_parts = [], [], []
    for head in range(2):
        own = first if head == 0 else jnp.logical_not(first)
        head_values = jnp.where(own, values, jnp.zeros_like(values))
        probs_low = probs_ref[head]
        probs = probs_low.astype(jnp.float32)
        grad_probs = lax.dot_general(head_values, grad_ctx, (((1,), (1,)), ((), ())), preferred_element_type=jnp.float32)
        row_dot = jnp.sum(probs * grad_probs, axis=0, keepdims=True)
        grad_scores = (probs * (grad_probs - row_dot)).astype(jnp.bfloat16)
        gv_parts.append(jnp.dot(probs_low, grad_ctx, preferred_element_type=jnp.float32))
        gk_parts.append(jnp.dot(grad_scores, queries, preferred_element_type=jnp.float32))
        gq_parts.append(jnp.dot(keys_t[head * HEAD_DIM : (head + 1) * HEAD_DIM], grad_scores, preferred_element_type=jnp.float32))
    col = pl.multiple_of(pl.program_id(1) * PAIR, PAIR)
    out_ref[:, pl.ds(col, PAIR)] = (jnp.concatenate(gq_parts, axis=0).T * scale).astype(jnp.bfloat16)
    out_ref[:, pl.ds(width + col, PAIR)] = (jnp.where(first, gk_parts[0], gk_parts[1]) * scale).astype(jnp.bfloat16)
    out_ref[:, pl.ds(2 * width + col, PAIR)] = jnp.where(first, gv_parts[0], gv_parts[1]).astype(jnp.bfloat16)

def attend_backward(projected, grad_context, probs, seq_count, seq_len, width, scale):
    pairs = width // PAIR
    return pl.pallas_call(
        partial(attend_backward_kernel, scale=scale), grid=(seq_count, pairs),
        in_specs=[
            pl.BlockSpec((seq_len, PAIR), lambda s, h: (s, h)),
            pl.BlockSpec((seq_len, PAIR), lambda s, h: (s, pairs + h)),
            pl.BlockSpec((seq_len, PAIR), lambda s, h: (s, 2 * pairs + h)),
            pl.BlockSpec((seq_len, PAIR), lambda s, h: (s, h)),
            pl.BlockSpec((2, seq_len, seq_len), lambda s, h: (s * pairs + h, 0, 0)),
        ],
        out_specs=pl.BlockSpec((seq_len, 3 * width), lambda s, h: (s, 0)),
        out_shape=jax.ShapeDtypeStruct((seq_count * seq_len, 3 * width), jnp.bfloat16),
        compiler_params=pltpu.CompilerParams(dimension_semantics=("arbitrary", "arbitrary")),
        name="attend_backward",
    )(projected, projected, projected, grad_context, probs)


def gather_kernel(layout, z_count, *refs):
    count = len(layout)
    local = refs[:count]
    whole = refs[count : 2 * count]
    send_sem, recv_sem, own_sem = refs[2 * count :]
    rep = lax.axis_index("rep")
    shard = lax.axis_index("shard")
    z, y = shard // 2, shard % 2
    core = rep % 2
    side = (rep // 2) % 2
    peer_core = rep + 1 - 2 * core
    peer_side = rep + 2 - 4 * side
    peer_y = shard + 1 - 2 * y
    has_up, has_down = z + 1 < z_count, z > 0

    barrier = pltpu.get_barrier_semaphore()
    def greet(target, amount=1):
        pl.semaphore_signal(barrier, inc=amount, device_id=target, device_id_type=MESH)
    greet((peer_core, shard))
    greet((peer_side, shard))
    greet((rep, peer_y))
    @pl.when(has_up)
    def _():
        greet((rep, shard + 2))
    @pl.when(has_down)
    def _():
        greet((rep, shard - 2))
    pl.semaphore_wait(barrier, 3 + has_up.astype(jnp.int32) + has_down.astype(jnp.int32))

    def part(group, ref, first, shards, owner_core, owner_side):
        split, share, across = layout[group]
        index = owner_side * 2 + owner_core if across else owner_core
        start = pl.multiple_of(index * share, share)
        rows = pl.ds(first, shards)
        if split == "columns":
            return ref.at[rows, :, pl.ds(start, share)]
        if split == "rows":
            return ref.at[rows, pl.ds(start, share), :]
        return ref.at[rows]

    slot_y, slot_x, slot_own, slot_far = (2 * z_count + i * z_count for i in range(4))

    def copy(group, source, first, shards, owner_core, owner_side, slot, target):
        return pltpu.make_async_remote_copy(
            src_ref=part(group, source, first, shards, owner_core, owner_side),
            dst_ref=part(group, whole[group], first, shards, owner_core, owner_side),
            send_sem=send_sem.at[group, slot],
            recv_sem=recv_sem.at[group, slot],
            device_id=target,
            device_id_type=MESH,
        )

    def own_part(group):
        return part(group, local[group], 0, 1, core, side)

    def keep_own(group):
        return pltpu.make_async_copy(
            own_part(group), part(group, whole[group], shard, 1, core, side), own_sem.at[group]
        )

    def along(group, origin, distance, up):
        slot = (0 if up else z_count) + distance
        source = whole[group]
        if distance == 0:
            src = own_part(group)
        else:
            src = part(group, source, origin * 2 + y, 1, core, side)
        return pltpu.make_async_remote_copy(
            src_ref=src, dst_ref=part(group, whole[group], origin * 2 + y, 1, core, side),
            send_sem=send_sem.at[group, slot], recv_sem=recv_sem.at[group, slot],
            device_id=(rep, shard + 2 if up else shard - 2), device_id_type=MESH)

    def to_y(group, origin, own):
        if own:
            src = own_part(group)
        else:
            src = part(group, whole[group], origin * 2 + y, 1, core, side)
        return pltpu.make_async_remote_copy(
            src_ref=src, dst_ref=part(group, whole[group], origin * 2 + y, 1, core, side),
            send_sem=send_sem.at[group, slot_y + origin], recv_sem=recv_sem.at[group, slot_y + origin],
            device_id=(rep, peer_y), device_id_type=MESH)

    def from_y(group, origin):
        dst = part(group, whole[group], origin * 2 + 1 - y, 1, core, side)
        return pltpu.make_async_remote_copy(
            src_ref=dst, dst_ref=dst,
            send_sem=send_sem.at[group, slot_y + origin], recv_sem=recv_sem.at[group, slot_y + origin],
            device_id=(rep, peer_y), device_id_type=MESH)

    def to_x(group, origin, mine):
        return copy(group, whole[group], origin * 2, 2, core, side if mine else 1 - side, slot_x + origin, (peer_side, shard))

    def to_core(group, origin, mine_core, mine_side):
        return copy(group, whole[group], origin * 2, 2, core if mine_core else 1 - core, side if mine_side else 1 - side,
                    (slot_own if mine_side else slot_far) + origin, (peer_core, shard))

    steps = [(d, up) for d in range(1, z_count) for up in (True, False)]

    def valid(d, up):
        return z - d >= 0 if up else z + d < z_count

    for group in range(count):
        keep_own(group).start()
    for group in range(count):
        @pl.when(has_up)
        def _(group=group):
            along(group, z, 0, True).start()
        @pl.when(has_down)
        def _(group=group):
            along(group, z, 0, False).start()
        to_y(group, z, True).start()
    for group in range(count):
        keep_own(group).wait()

    def finish_pair(group, origin):
        from_y(group, origin).wait_recv()
        split, share, across = layout[group]
        if across:
            to_x(group, origin, True).start()
        if split is not None:
            to_core(group, origin, True, True).start()

    for group in range(count):
        across = layout[group][2]
        pending = []
        for d, up in steps:
            origin = z - d if up else z + d
            @pl.when(valid(d, up))
            def _(group=group, d=d, up=up, origin=origin):
                along(group, origin, d - 1, up).wait_recv()
                further = has_up if up else has_down
                if d < z_count - 1:
                    @pl.when(further)
                    def _():
                        along(group, origin, d, up).start()
                to_y(group, origin, False).start()
            if d == 1 and not up:
                finish_pair(group, z)
            if d > 1 and not up:
                for u in (True, False):
                    o = z - d + 1 if u else z + d - 1
                    @pl.when(valid(d - 1, u))
                    def _(group=group, o=o):
                        finish_pair(group, o)
        d = z_count - 1
        for u in (True, False):
            o = z - d if u else z + d
            @pl.when(valid(d, u))
            def _(group=group, o=o):
                finish_pair(group, o)

    order = [(0, True)] + steps
    def each(fn):
        for d, up in order:
            o = z - d if up else z + d
            if d == 0:
                fn(o)
            else:
                @pl.when(valid(d, up))
                def _(o=o):
                    fn(o)
    for group in range(count):
        if layout[group][2]:
            def relay(o, group=group):
                to_x(group, o, False).wait_recv()
                to_core(group, o, True, False).start()
            each(relay)
    for group in range(count):
        split, share, across = layout[group]
        def last(o, group=group, split=split, across=across):
            if split is not None:
                to_core(group, o, False, True).wait_recv()
            if across:
                to_core(group, o, False, False).wait_recv()
        each(last)
    for group in range(count):
        split, share, across = layout[group]
        @pl.when(has_up)
        def _(group=group):
            along(group, z, 0, True).wait_send()
        @pl.when(has_down)
        def _(group=group):
            along(group, z, 0, False).wait_send()
        for d, up in steps:
            if d < z_count - 1:
                origin = z - d if up else z + d
                @pl.when(jnp.logical_and(valid(d, up), has_up if up else has_down))
                def _(group=group, d=d, up=up, origin=origin):
                    along(group, origin, d, up).wait_send()
        def sent(o, group=group, split=split, across=across):
            to_y(group, o, False).wait_send()
            if across:
                to_x(group, o, True).wait_send()
                to_core(group, o, True, False).wait_send()
            if split is not None:
                to_core(group, o, True, True).wait_send()
        each(sent)

def gather_all(local, layout, shards, collective_id, cost=0):
    count = len(local)
    z_count = shards // 2
    slots = 6 * z_count
    return pl.pallas_call(
        partial(gather_kernel, layout, z_count),
        out_shape=[jax.ShapeDtypeStruct((shards,) + a.shape, a.dtype) for a in local],
        in_specs=[pl.BlockSpec(memory_space=pltpu.VMEM)] * count,
        out_specs=[pl.BlockSpec(memory_space=pl.ANY)] * count,
        scratch_shapes=[pltpu.SemaphoreType.DMA((count, slots)), pltpu.SemaphoreType.DMA((count, slots)), pltpu.SemaphoreType.DMA((count,))],
        compiler_params=pltpu.CompilerParams(collective_id=collective_id, has_side_effects=True),
        name="gather_weights",
        cost_estimate=pl.CostEstimate(flops=0, bytes_accessed=cost, transcendentals=0),
    )(*[a[None] for a in local])


def swap(value, bit):
    count = lax.axis_size("rep")
    return lax.ppermute(value, "rep", [(i, i ^ bit) for i in range(count)])


def pick(values, bit_value):
    return jnp.where(bit_value == 0, values[0], values[1])


def reduce_weight(pieces, core, side):
    shards = pieces[0][0].shape[0]
    both = jnp.stack([jnp.stack(pieces[0]), jnp.stack(pieces[1])])
    send = lax.dynamic_index_in_dim(both, 1 - core, 1, keepdims=False)
    keep = lax.dynamic_index_in_dim(both, core, 1, keepdims=False)
    arrived = swap(send, 1)
    far = 1 - side
    send = (
        lax.dynamic_index_in_dim(keep, far, 0, keepdims=False).astype(jnp.float32)
        + lax.dynamic_index_in_dim(arrived, far, 0, keepdims=False).astype(jnp.float32)
    ).astype(jnp.bfloat16)
    near = lax.dynamic_index_in_dim(keep, side, 0, keepdims=False).astype(
        jnp.float32
    ) + lax.dynamic_index_in_dim(arrived, side, 0, keepdims=False).astype(jnp.float32)
    summed = (near + swap(send, 2).astype(jnp.float32)).astype(jnp.bfloat16)
    spread = lax.all_to_all(summed, "shard", split_axis=0, concat_axis=0, tiled=True)
    total = jnp.sum(spread.astype(jnp.float32), axis=0).astype(jnp.bfloat16)
    bit = 4
    while bit < lax.axis_size("rep"):
        total = (total.astype(jnp.float32) + swap(total, bit).astype(jnp.float32)).astype(jnp.bfloat16)
        bit *= 2
    other_side = swap(total, 2)
    mine = jnp.stack([total, other_side])
    theirs = swap(mine, 1)
    by_core = [jnp.where(core == 0, mine, theirs), jnp.where(core == 0, theirs, mine)]
    quarters = []
    for s in range(2):
        for c in range(2):
            quarters.append(jnp.where(side == s, by_core[c][0], by_core[c][1]))
    return quarters


def by_columns(grad, shards):
    rows, columns = grad.shape
    quarter = columns // 4
    cut = [grad[:, i * quarter : (i + 1) * quarter].reshape(shards, rows // shards, quarter) for i in range(4)]
    return [[cut[0], cut[1]], [cut[2], cut[3]]]


def by_rows(grad, shards):
    rows, columns = grad.shape
    quarter = rows // shards // 4
    cut = grad.reshape(shards, 4, quarter, columns)
    return [[cut[:, 0], cut[:, 1]], [cut[:, 2], cut[:, 3]]]


def per_device(
    tokens,
    lengths,
    seq_order,
    w_query,
    w_key,
    w_value,
    w_out,
    b_query,
    b_value,
    b_out,
    ln1_gain,
    ln1_bias,
    w_up,
    b_up,
    w_down,
    b_down,
    ln2_gain,
    ln2_bias,
    cotangent,
):
    device_count = lax.axis_size(("rep", "shard"))
    shards = lax.axis_size("shard")
    core = lax.axis_index("rep") % 2
    side = (lax.axis_index("rep") // 2) % 2
    seq_count, seq_len, model_width = cotangent.shape
    hidden_width = w_up.shape[1]
    part_len = tokens.shape[1]
    score_scale = float(model_width // HEADS) ** (-0.5)
    row_count = seq_count * seq_len
    slot_table = seq_order.reshape(device_count, seq_count).T
    picked = tokens[slot_table]
    arrived = lax.all_to_all(picked, ("rep", "shard"), split_axis=1, concat_axis=1, tiled=True)
    tok_rows = arrived.reshape(row_count, model_width)
    my_index = lax.axis_index(("rep", "shard"))
    my_slots = lax.dynamic_slice_in_dim(seq_order, my_index * seq_count, seq_count)
    my_lengths = lengths[my_slots]
    key_mask = jnp.arange(seq_len, dtype=jnp.int32)[None, :] < my_lengths[:, None]
    valid_rows = key_mask.reshape(row_count, 1).astype(jnp.float32)

    w_attn = jnp.concatenate([w_query, w_key, w_value, w_out], axis=1)
    vectors = (b_query, b_value, b_out, ln1_gain, ln1_bias, b_down, ln2_gain, ln2_bias, b_up)
    packed = jnp.concatenate(vectors)
    room = 16 * PAIR
    packed = jnp.pad(packed, (0, room - packed.shape[0])).reshape(16, PAIR)
    layout = (
        ("columns", model_width, True),
        ("columns", hidden_width // 4, True),
        ("rows", w_down.shape[0] // 2, False),
        (None, 0, False),
    )
    all_attn, all_up, all_down, all_small = gather_all(
        (w_attn, w_up, w_down, packed), layout, shards, collective_id=1, cost=100 << 20
    )
    all_attn = all_attn.reshape(model_width, 4 * model_width)
    all_up = all_up.reshape(model_width, hidden_width)
    all_down = all_down.reshape(hidden_width, model_width)
    flat = all_small.reshape(shards, room).astype(jnp.float32)
    small = []
    at = 0
    for vector in vectors:
        size = vector.shape[0]
        small.append(flat[:, at : at + size].reshape(shards * size))
        at += size
    f_b_query, f_b_value, f_b_out, gain_one, f_ln1_bias, f_b_down, gain_two, f_ln2_bias, f_b_up = small

    w_in = all_attn[:, : 3 * model_width]
    w_out_all = all_attn[:, 3 * model_width :]
    bias_in = jnp.concatenate([f_b_query, jnp.zeros_like(f_b_query), f_b_value])
    projected = (jnp.dot(tok_rows, w_in, preferred_element_type=jnp.float32) + bias_in).astype(jnp.bfloat16)
    context, probs = attend_forward(projected, my_lengths, seq_count, seq_len, model_width, score_scale)
    attn_out = jnp.dot(context, w_out_all, preferred_element_type=jnp.float32) + f_b_out
    resid_one = tok_rows.astype(jnp.float32) + attn_out
    normed_one, inv_one = norm_stats(resid_one)
    hidden_one = normed_one * gain_one + f_ln1_bias
    hidden_low = hidden_one.astype(jnp.bfloat16)
    up_proj = jnp.dot(hidden_low, all_up, preferred_element_type=jnp.float32) + f_b_up
    activated, gelu_pull = jax.vjp(exact_gelu, up_proj)
    act_low = activated.astype(jnp.bfloat16)
    ffn_out = jnp.dot(act_low, all_down, preferred_element_type=jnp.float32) + f_b_down
    resid_two = hidden_one + ffn_out
    normed_two, inv_two = norm_stats(resid_two)
    result_rows = normed_two * gain_two + f_ln2_bias
    outputs = result_rows.astype(jnp.bfloat16).reshape(seq_count, seq_len, model_width)
    grad_out = cotangent.reshape(row_count, model_width).astype(jnp.float32) * valid_rows
    d_ln2_gain = jnp.sum(grad_out * normed_two, axis=0)
    d_ln2_bias = jnp.sum(grad_out, axis=0)
    grad_resid_two = norm_back(grad_out, normed_two, inv_two, gain_two)
    grad_ffn = grad_resid_two.astype(jnp.bfloat16)
    d_w_down = contract_rows(act_low, grad_ffn).astype(jnp.bfloat16)
    down_quarters = reduce_weight(by_rows(d_w_down, shards), core, side)
    d_b_down = jnp.sum(grad_ffn.astype(jnp.float32), axis=0)
    grad_act = contract_cols(grad_ffn, all_down)
    grad_up = gelu_pull(grad_act)[0].astype(jnp.bfloat16)
    d_w_up = contract_rows(hidden_low, grad_up).astype(jnp.bfloat16)
    up_quarters = reduce_weight(by_columns(d_w_up, shards), core, side)
    d_b_up = jnp.sum(grad_up.astype(jnp.float32), axis=0)
    grad_hidden = grad_resid_two + contract_cols(grad_up, all_up)
    d_ln1_gain = jnp.sum(grad_hidden * normed_one, axis=0)
    d_ln1_bias = jnp.sum(grad_hidden, axis=0)
    grad_resid_one = norm_back(grad_hidden, normed_one, inv_one, gain_one)
    grad_attn = grad_resid_one.astype(jnp.bfloat16)
    d_w_out = contract_rows(context, grad_attn).astype(jnp.bfloat16)
    d_b_out = jnp.sum(grad_attn.astype(jnp.float32), axis=0)
    grad_context = contract_cols(grad_attn, w_out_all).astype(jnp.bfloat16)
    grad_projected = attend_backward(projected, grad_context, probs, seq_count, seq_len, model_width, score_scale)
    grad_rows = grad_resid_one + contract_cols(grad_projected, w_in)
    back_rows = grad_rows.astype(jnp.bfloat16).reshape(seq_count, device_count, part_len, model_width)
    returned = lax.all_to_all(back_rows, ("rep", "shard"), split_axis=1, concat_axis=1, tiled=True)
    d_w_in = contract_rows(tok_rows, grad_projected).astype(jnp.bfloat16)
    attn_quarters = reduce_weight(
        by_columns(jnp.concatenate([d_w_in, d_w_out], axis=1), shards), core, side
    )
    grad_wide = grad_projected.astype(jnp.float32)
    d_b_query = jnp.sum(grad_wide[:, :model_width], axis=0)
    d_b_value = jnp.sum(grad_wide[:, 2 * model_width :], axis=0)
    d_small = (d_b_query, d_b_value, d_b_out, d_ln1_gain, d_ln1_bias, d_b_down, d_ln2_gain, d_ln2_bias, d_b_up)
    rows = jnp.concatenate([d.reshape(shards, -1) for d in d_small], axis=1)
    rows = jnp.pad(rows, ((0, 0), (0, room - rows.shape[1]))).reshape(shards, 16, PAIR)
    spread = lax.all_to_all(rows, "shard", split_axis=0, concat_axis=0, tiled=True)
    total = jnp.sum(spread, axis=0)
    bit = 1
    while bit < lax.axis_size("rep"):
        total = total + swap(total, bit)
        bit *= 2
    total = total.reshape(room)
    small_out = []
    at = 0
    for vector in vectors:
        size = vector.shape[0]
        small_out.append(total[at : at + size])
        at += size
    g_b_query, g_b_value, g_b_out, g_ln1_gain, g_ln1_bias, g_b_down, g_ln2_gain, g_ln2_bias, g_b_up = small_out

    every = jnp.arange(seq_order.shape[0], dtype=jnp.int32)
    slot_of = jnp.sum(jnp.where(seq_order[None, :] == every[:, None], every[None, :], 0), axis=1)
    by_slot = returned.transpose(1, 0, 2, 3).reshape(device_count * seq_count, part_len, model_width)
    grad_tokens = by_slot[slot_of]
    g_up = jnp.concatenate(up_quarters, axis=1).astype(jnp.float32)
    g_down = jnp.concatenate(down_quarters, axis=0).astype(jnp.float32)
    g_attn = [q.astype(jnp.float32) for q in attn_quarters]
    return (
        outputs,
        grad_tokens,
        *g_attn,
        g_b_query,
        g_b_value,
        g_b_out,
        g_ln1_gain,
        g_ln1_bias,
        g_up,
        g_b_up,
        g_down,
        g_b_down,
        g_ln2_gain,
        g_ln2_bias,
    )


def solution(mesh):
    in_specs = (
        P(None, ("rep", "shard"), None),
        P(),
        P(),
        P("shard", None),
        P("shard", None),
        P("shard", None),
        P("shard", None),
        P("shard"),
        P("shard"),
        P("shard"),
        P("shard"),
        P("shard"),
        P("shard", None),
        P("shard"),
        P("shard", None),
        P("shard"),
        P("shard"),
        P("shard"),
        P(("rep", "shard"), None, None),
    )
    out_specs = (
        P(("rep", "shard"), None, None),
        P(None, ("rep", "shard"), None),
        P("shard", None),
        P("shard", None),
        P("shard", None),
        P("shard", None),
        P("shard"),
        P("shard"),
        P("shard"),
        P("shard"),
        P("shard"),
        P("shard", None),
        P("shard"),
        P("shard", None),
        P("shard"),
        P("shard"),
        P("shard"),
    )
    return jax.shard_map(
        per_device, mesh=mesh, in_specs=in_specs, out_specs=out_specs, check_vma=False
    )
```

```python
from functools import partial

import jax
import jax.numpy as jnp
from jax import lax
from jax.experimental import pallas as pl
from jax.experimental.pallas import tpu as pltpu
from jax.sharding import PartitionSpec as P

HEADS = 12
HEAD_DIM = 64
PAIR = 128
NEG_FILL = -1e30
EPS_NORM = 1e-12
LOG2E = 1.4426950408889634
MESH = pl.DeviceIdType.MESH


def contract_rows(left, right):
    return lax.dot_general(
        left, right, (((0,), (0,)), ((), ())), preferred_element_type=jnp.float32
    )


def contract_cols(left, right):
    return lax.dot_general(
        left, right, (((1,), (1,)), ((), ())), preferred_element_type=jnp.float32
    )


def norm_stats(resid):
    row_mean = jnp.mean(resid, axis=-1, keepdims=True)
    centered = resid - row_mean
    variance = jnp.mean(centered * centered, axis=-1, keepdims=True)
    inv_std = lax.rsqrt(variance + EPS_NORM)
    return (centered * inv_std, inv_std)


def norm_back(grad_in, normed, inv_std, gain):
    scaled = grad_in * gain
    mean_grad = jnp.mean(scaled, axis=-1, keepdims=True)
    mean_cross = jnp.mean(scaled * normed, axis=-1, keepdims=True)
    return inv_std * (scaled - mean_grad - normed * mean_cross)


def exact_gelu(values):
    return jax.nn.gelu(values, approximate=False)


class Spot:
    def __init__(self, z_count):
        self.rep, self.shard = lax.axis_index("rep"), lax.axis_index("shard")
        self.z_count = z_count
        self.core, self.side = self.rep % 2, (self.rep // 2) % 2
        self.y, self.z = self.shard % 2, self.shard // 2
        core_step, side_step = 1 - 2 * self.core, 2 - 4 * self.side
        self.over_core = (self.rep + core_step, self.shard)
        self.over_x = (self.rep + side_step, self.shard)
        self.over_y = (self.rep, self.shard + 1 - 2 * self.y)

    def z_after(self, step):
        return lax.rem(self.z + step, self.z_count)

    def ahead(self, step):
        return (self.rep, 2 * self.z_after(step) + self.y)

    def greet(self):
        barrier = pltpu.get_barrier_semaphore()
        targets = [self.over_core, self.over_x, self.over_y]
        targets += [self.ahead(step) for step in range(1, self.z_count)]
        for target in targets:
            pl.semaphore_signal(barrier, inc=1, device_id=target, device_id_type=MESH)
        pl.semaphore_wait(barrier, len(targets))


def sum_slots(z_count):
    return 7 * z_count + 3


def sum_scratch(z_count, rows, columns):
    low = jnp.bfloat16
    return [
        pltpu.VMEM((z_count, 2, 2, rows, columns), low),
        pltpu.VMEM((z_count, 2, 2, rows, columns), low),
        pltpu.VMEM((z_count, 2, rows, columns), low),
        pltpu.VMEM((z_count, rows, columns), low),
        pltpu.VMEM((z_count, rows, columns), low),
        pltpu.VMEM((rows, columns), low),
        pltpu.SemaphoreType.DMA((sum_slots(z_count),)),
        pltpu.SemaphoreType.DMA((sum_slots(z_count),)),
        pltpu.SemaphoreType.DMA((4 * z_count + 1,)),
    ]


class WeightSum:
    def __init__(self, spot, grad, result, pattern, scratch):
        self.spot, self.grad, self.result, self.pattern = spot, grad, result, pattern
        self.own, self.core_in, self.wide_in, self.thin_in, self.line_in, self.total = scratch[:6]
        self.send_sem, self.recv_sem, self.load_sem = scratch[6:]
        self.count = spot.z_count
        self.quarter = 2 * spot.side + spot.core

    def x_first(self, i):
        return self.pattern[i % len(self.pattern)] == "x"

    def block(self, shard, quarter):
        if len(self.grad.shape) == 4:
            return self.grad.at[shard, quarter]
        width = self.total.shape[1]
        return self.grad.at[shard, :, pl.ds(pl.multiple_of(quarter * width, width), width)]

    def remote(self, slot, source, target_ref, device):
        return pltpu.make_async_remote_copy(
            src_ref=source, dst_ref=target_ref, send_sem=self.send_sem.at[slot], recv_sem=self.recv_sem.at[slot],
            device_id=device, device_id_type=MESH)

    def place(self, i, s, y):
        spot = self.spot
        shard = 2 * spot.z_after(i + 1) + (spot.y if y else 1 - spot.y)
        return shard, 2 * (spot.side if s else 1 - spot.side)

    def to_core(self, i, s, y):
        shard, base = self.place(i, s, y)
        return self.remote(4 * i + 2 * s + y, self.block(shard, base + 1 - self.spot.core), self.core_in.at[i, s, y], self.spot.over_core)

    def load(self, i, s, y):
        shard, base = self.place(i, s, y)
        return pltpu.make_async_copy(self.block(shard, base + self.spot.core), self.own.at[i, s, y], self.load_sem.at[4 * i + 2 * s + y])

    def wide(self, i):
        source = self.own.at[i, 0] if self.x_first(i) else self.own.at[i, :, 0]
        return self.remote(4 * self.count + i, source, self.wide_in.at[i], self.spot.over_x if self.x_first(i) else self.spot.over_y)

    def thin(self, i):
        source = self.own.at[i, 1, 0] if self.x_first(i) else self.own.at[i, 0, 1]
        return self.remote(5 * self.count + i, source, self.thin_in.at[i], self.spot.over_y if self.x_first(i) else self.spot.over_x)

    def line(self, i):
        return self.remote(6 * self.count + i, self.own.at[i, 1, 1], self.line_in.at[i], self.spot.ahead(i + 1))

    def keep(self):
        return pltpu.make_async_copy(self.total, self.result.at[self.quarter], self.load_sem.at[4 * self.count])

    def spread(self, which, arriving=False):
        spot = self.spot
        far_core, far_side = (arriving and which != 1), (which == 2 or (arriving and which == 1))
        core = 1 - spot.core if far_core else spot.core
        side = 1 - spot.side if far_side else spot.side
        there = self.result.at[2 * side + core]
        source = there if which == 2 else self.total
        return self.remote(7 * self.count + which, source, there, spot.over_x if which == 1 else spot.over_core)

    def begin(self):
        for i in range(self.count):
            for s in range(2):
                for y in range(2):
                    self.to_core(i, s, y).start()
                    self.load(i, s, y).start()

    def add_core(self, i, s, y):
        self.to_core(i, s, y).wait_recv()
        self.load(i, s, y).wait()
        self.own[i, s, y] = self.own[i, s, y] + self.core_in[i, s, y]

    def step_wide(self, i):
        for other in range(2):
            self.add_core(i, *((0, other) if self.x_first(i) else (other, 0)))
        self.wide(i).start()
        for other in range(2):
            self.add_core(i, *((1, other) if self.x_first(i) else (other, 1)))

    def step_thin(self, i):
        self.wide(i).wait_recv()
        for other in range(2):
            at = (1, other) if self.x_first(i) else (other, 1)
            self.own[i, at[0], at[1]] = self.own[i, at[0], at[1]] + self.wide_in[i, other]
            if other == 0:
                self.thin(i).start()

    def step_line(self, i):
        self.thin(i).wait_recv()
        self.own[i, 1, 1] = self.own[i, 1, 1] + self.thin_in[i]
        if i < self.count - 1:
            self.line(i).start()

    def step_total(self):
        total = self.own[self.count - 1, 1, 1].astype(jnp.float32)
        for i in range(self.count - 1):
            self.line(i).wait_recv()
            total = total + self.line_in[i].astype(jnp.float32)
        self.total[...] = total.astype(jnp.bfloat16)
        self.keep().start()
        self.spread(1).start()
        self.spread(0).start()

    def step_relay(self):
        self.spread(1, True).wait_recv()
        self.spread(2).start()

    def end(self):
        self.spread(0, True).wait_recv()
        self.spread(2, True).wait_recv()
        self.keep().wait()
        for i in range(self.count):
            for s in range(2):
                for y in range(2):
                    self.to_core(i, s, y).wait_send()
            self.wide(i).wait_send()
            self.thin(i).wait_send()
            if i < self.count - 1:
                self.line(i).wait_send()
        for which in range(3):
            self.spread(which).wait_send()


class VectorSum:
    def __init__(self, spot, local, result, scratch):
        self.spot, self.local, self.result = spot, local, result
        self.core_in, self.x_in, self.y_in, self.line_in, self.core_sum, self.x_sum, self.y_sum = scratch[:7]
        self.send_sem, self.recv_sem = scratch[7:]

    def remote(self, slot, source, target_ref, device):
        return pltpu.make_async_remote_copy(
            src_ref=source, dst_ref=target_ref, send_sem=self.send_sem.at[slot], recv_sem=self.recv_sem.at[slot],
            device_id=device, device_id_type=MESH)

    def to_core(self):
        return self.remote(0, self.local, self.core_in, self.spot.over_core)

    def to_x(self):
        return self.remote(1, self.core_sum, self.x_in, self.spot.over_x)

    def to_y(self):
        return self.remote(2, self.x_sum.at[:, 1 - self.spot.y], self.y_in, self.spot.over_y)

    def line(self, i):
        return self.remote(3 + i, self.y_sum.at[self.spot.z_after(i + 1)], self.line_in.at[i], self.spot.ahead(i + 1))

    def begin(self):
        self.to_core().start()

    def step_x(self):
        self.to_core().wait_recv()
        self.core_sum[...] = self.local[...] + self.core_in[...]
        self.to_x().start()

    def step_y(self):
        self.to_x().wait_recv()
        self.x_sum[...] = self.core_sum[...] + self.x_in[...]
        self.to_y().start()

    def step_line(self):
        self.to_y().wait_recv()
        self.y_sum[...] = self.x_sum[:, self.spot.y] + self.y_in[...]
        for i in range(self.spot.z_count - 1):
            self.line(i).start()

    def step_total(self):
        total = self.y_sum[self.spot.z]
        for i in range(self.spot.z_count - 1):
            self.line(i).wait_recv()
            total = total + self.line_in[i]
        self.result[...] = total

    def end(self):
        self.to_core().wait_send()
        self.to_x().wait_send()
        self.to_y().wait_send()
        for i in range(self.spot.z_count - 1):
            self.line(i).wait_send()


def vector_scratch(z_count):
    pair, single = (z_count, 2, 16, PAIR), (z_count, 16, PAIR)
    shapes = (pair, pair, single, single, pair, pair, single)
    return [pltpu.VMEM(shape, jnp.float32) for shape in shapes] + [
        pltpu.SemaphoreType.DMA((3 + z_count,)), pltpu.SemaphoreType.DMA((3 + z_count,))]


def reduce_kernel(grad, vectors, result, vector_result, *scratch):
    z_count = vectors.shape[0]
    spot = Spot(z_count)
    spot.greet()
    weight = WeightSum(spot, grad, result, "xy", scratch[:9])
    vector = VectorSum(spot, vectors, vector_result, scratch[9:])
    weight.begin()
    vector.begin()
    for i in range(z_count):
        weight.step_wide(i)
        if i == 0:
            vector.step_x()
        if i == 2:
            vector.step_y()
    for i in range(z_count):
        weight.step_thin(i)
        if i > 0:
            weight.step_line(i - 1)
        if i == 0:
            vector.step_line()
    vector.step_total()
    weight.step_line(z_count - 1)
    weight.step_total()
    weight.step_relay()
    weight.end()
    vector.end()


def reduce_last(grad, vectors, shards, collective_id):
    z_count = shards // 2
    rows, columns = grad.shape[0] // shards, grad.shape[1] // 4
    return pl.pallas_call(
        reduce_kernel,
        out_shape=[jax.ShapeDtypeStruct((4, rows, columns), jnp.bfloat16), jax.ShapeDtypeStruct((16, PAIR), jnp.float32)],
        in_specs=[pl.BlockSpec(memory_space=pl.ANY), pl.BlockSpec(memory_space=pltpu.VMEM)],
        out_specs=[pl.BlockSpec(memory_space=pl.ANY), pl.BlockSpec(memory_space=pltpu.VMEM)],
        scratch_shapes=sum_scratch(z_count, rows, columns) + vector_scratch(z_count),
        compiler_params=pltpu.CompilerParams(collective_id=collective_id, has_side_effects=True),
        name="reduce_last",
        cost_estimate=pl.CostEstimate(flops=0, bytes_accessed=100 << 20, transcendentals=0),
    )(grad.reshape(shards, rows, 4 * columns), vectors.reshape(z_count, 2, 16, PAIR))


def attend_forward_kernel(len_ref, q_ref, k_ref, v_ref, ctx_ref, probs_ref, *, scale):
    seq_len = q_ref.shape[0]
    valid = len_ref[pl.program_id(0)]
    key_pos = lax.broadcasted_iota(jnp.int32, (seq_len, PAIR), 0)
    fill = jnp.where(key_pos < valid, 0.0, NEG_FILL)[:, :1]
    first = lax.broadcasted_iota(jnp.int32, (seq_len, PAIR), 1) < HEAD_DIM
    queries = q_ref[...]
    keys = k_ref[...]
    values_t = v_ref[...].T
    parts = []
    for head in range(2):
        own = first if head == 0 else jnp.logical_not(first)
        head_keys = jnp.where(own, keys, jnp.zeros_like(keys))
        scores = lax.dot_general(head_keys, queries, (((1,), (1,)), ((), ())), preferred_element_type=jnp.float32)
        scaled = scores * (scale * LOG2E) + fill
        top = jnp.max(scaled, axis=0, keepdims=True)
        raised = jnp.exp2(scaled - top)
        total = jnp.sum(raised, axis=0, keepdims=True)
        probs = (raised * (1.0 / total)).astype(jnp.bfloat16)
        probs_ref[head] = probs
        parts.append(jnp.dot(values_t[head * HEAD_DIM : (head + 1) * HEAD_DIM], probs, preferred_element_type=jnp.float32))
    ctx_ref[...] = jnp.concatenate(parts, axis=0).T.astype(jnp.bfloat16)

def attend_forward(projected, lens, seq_count, seq_len, width, scale):
    pairs = width // PAIR
    grid_spec = pltpu.PrefetchScalarGridSpec(
        num_scalar_prefetch=1, grid=(seq_count, pairs),
        in_specs=[
            pl.BlockSpec((seq_len, PAIR), lambda s, h, n: (s, h)),
            pl.BlockSpec((seq_len, PAIR), lambda s, h, n: (s, pairs + h)),
            pl.BlockSpec((seq_len, PAIR), lambda s, h, n: (s, 2 * pairs + h)),
        ],
        out_specs=[
            pl.BlockSpec((seq_len, PAIR), lambda s, h, n: (s, h)),
            pl.BlockSpec((2, seq_len, seq_len), lambda s, h, n: (s * pairs + h, 0, 0)),
        ])
    return pl.pallas_call(
        partial(attend_forward_kernel, scale=scale), grid_spec=grid_spec,
        out_shape=[jax.ShapeDtypeStruct((seq_count * seq_len, width), jnp.bfloat16),
                   jax.ShapeDtypeStruct((seq_count * 2 * pairs, seq_len, seq_len), jnp.bfloat16)],
        compiler_params=pltpu.CompilerParams(dimension_semantics=("arbitrary", "arbitrary")),
        name="attend_forward",
    )(lens, projected, projected, projected)

def attend_backward_kernel(q_ref, k_ref, v_ref, gctx_ref, probs_ref, up_ref, down_ref, out_ref, up_sum, down_sum, *scratch, scale, z_count):
    spot = Spot(z_count)
    up = WeightSum(spot, up_ref, up_sum, "xy", scratch[:9])
    down = WeightSum(spot, down_ref, down_sum, "yx", scratch[9:])
    def begin():
        spot.greet()
        down.begin()
        up.begin()

    turns = [begin] + [partial(weight.step_wide, i) for weight in (down, up) for i in range(z_count)]
    for weight in (down, up):
        for i in range(z_count):
            turns.append(partial(weight.step_thin, i))
            if i > 0:
                turns.append(partial(weight.step_line, i - 1))
        turns.append(partial(weight.step_line, z_count - 1))
    step = pl.program_id(0) * pl.num_programs(1) + pl.program_id(1)
    pairs = out_ref.shape[1] // 3 // PAIR
    placed = [0] + [2 + i // 2 for i in range(2 * z_count)]
    placed += [min(placed[-1] + 2 + i, 2 * pairs - 1) for i in range(len(turns) - len(placed))]
    for at in range(2 * pairs):
        due = [turn for turn, where in zip(turns, placed) if where == at]
        if due and at < 2 * pairs - 1:
            @pl.when(step == at)
            def _(due=due):
                for turn in due:
                    turn()

    seq_len = q_ref.shape[0]
    width = out_ref.shape[1] // 3
    first = lax.broadcasted_iota(jnp.int32, (seq_len, PAIR), 1) < HEAD_DIM
    queries = q_ref[...]
    keys_t = k_ref[...].T
    values = v_ref[...]
    grad_ctx = gctx_ref[...]
    gq_parts, gk_parts, gv_parts = [], [], []
    for head in range(2):
        own = first if head == 0 else jnp.logical_not(first)
        head_values = jnp.where(own, values, jnp.zeros_like(values))
        probs_low = probs_ref[head]
        probs = probs_low.astype(jnp.float32)
        grad_probs = lax.dot_general(head_values, grad_ctx, (((1,), (1,)), ((), ())), preferred_element_type=jnp.float32)
        row_dot = jnp.sum(probs * grad_probs, axis=0, keepdims=True)
        grad_scores = (probs * (grad_probs - row_dot)).astype(jnp.bfloat16)
        gv_parts.append(jnp.dot(probs_low, grad_ctx, preferred_element_type=jnp.float32))
        gk_parts.append(jnp.dot(grad_scores, queries, preferred_element_type=jnp.float32))
        gq_parts.append(jnp.dot(keys_t[head * HEAD_DIM : (head + 1) * HEAD_DIM], grad_scores, preferred_element_type=jnp.float32))
    col = pl.multiple_of(pl.program_id(1) * PAIR, PAIR)
    out_ref[:, pl.ds(col, PAIR)] = (jnp.concatenate(gq_parts, axis=0).T * scale).astype(jnp.bfloat16)
    out_ref[:, pl.ds(width + col, PAIR)] = (jnp.where(first, gk_parts[0], gk_parts[1]) * scale).astype(jnp.bfloat16)
    out_ref[:, pl.ds(2 * width + col, PAIR)] = jnp.where(first, gv_parts[0], gv_parts[1]).astype(jnp.bfloat16)

    @pl.when(step == pl.num_programs(0) * pl.num_programs(1) - 1)
    def _():
        for turn, where in zip(turns, placed):
            if where >= 2 * pairs - 1:
                turn()
        for weight in (down, up):
            weight.step_total()
        for weight in (down, up):
            weight.step_relay()
        for weight in (down, up):
            weight.end()


def attend_backward(projected, grad_context, probs, grad_up, grad_down, shards, seq_count, seq_len, width, scale, collective_id):
    pairs = width // PAIR
    z_count = shards // 2
    rows, columns = grad_up.shape[0] // shards, grad_up.shape[1] // 4
    low_rows, low_columns = grad_down.shape[0] // shards // 4, grad_down.shape[1]
    return pl.pallas_call(
        partial(attend_backward_kernel, scale=scale, z_count=z_count), grid=(seq_count, pairs),
        in_specs=[
            pl.BlockSpec((seq_len, PAIR), lambda s, h: (s, h)),
            pl.BlockSpec((seq_len, PAIR), lambda s, h: (s, pairs + h)),
            pl.BlockSpec((seq_len, PAIR), lambda s, h: (s, 2 * pairs + h)),
            pl.BlockSpec((seq_len, PAIR), lambda s, h: (s, h)),
            pl.BlockSpec((2, seq_len, seq_len), lambda s, h: (s * pairs + h, 0, 0)),
            pl.BlockSpec(memory_space=pl.ANY),
            pl.BlockSpec(memory_space=pl.ANY),
        ],
        out_specs=[
            pl.BlockSpec((seq_len, 3 * width), lambda s, h: (s, 0)),
            pl.BlockSpec(memory_space=pl.ANY),
            pl.BlockSpec(memory_space=pl.ANY),
        ],
        out_shape=[
            jax.ShapeDtypeStruct((seq_count * seq_len, 3 * width), jnp.bfloat16),
            jax.ShapeDtypeStruct((4, rows, columns), jnp.bfloat16),
            jax.ShapeDtypeStruct((4, low_rows, low_columns), jnp.bfloat16),
        ],
        scratch_shapes=sum_scratch(z_count, rows, columns) + sum_scratch(z_count, low_rows, low_columns),
        compiler_params=pltpu.CompilerParams(
            dimension_semantics=("arbitrary", "arbitrary"), collective_id=collective_id, has_side_effects=True),
        name="attend_backward",
        cost_estimate=pl.CostEstimate(flops=0, bytes_accessed=60 << 20, transcendentals=0),
    )(projected, projected, projected, grad_context, probs,
      grad_up.reshape(shards, rows, 4 * columns), grad_down.reshape(shards, 4, low_rows, low_columns))


def gather_kernel(layout, z_count, *refs):
    count = len(layout)
    local = refs[:count]
    whole = refs[count : 2 * count]
    send_sem, recv_sem, own_sem = refs[2 * count :]
    rep = lax.axis_index("rep")
    shard = lax.axis_index("shard")
    z, y = shard // 2, shard % 2
    core = rep % 2
    side = (rep // 2) % 2
    peer_core = rep + 1 - 2 * core
    peer_side = rep + 2 - 4 * side
    peer_y = shard + 1 - 2 * y
    has_up, has_down = z + 1 < z_count, z > 0

    barrier = pltpu.get_barrier_semaphore()
    def greet(target, amount=1):
        pl.semaphore_signal(barrier, inc=amount, device_id=target, device_id_type=MESH)
    greet((peer_core, shard))
    greet((peer_side, shard))
    greet((rep, peer_y))
    @pl.when(has_up)
    def _():
        greet((rep, shard + 2))
    @pl.when(has_down)
    def _():
        greet((rep, shard - 2))
    pl.semaphore_wait(barrier, 3 + has_up.astype(jnp.int32) + has_down.astype(jnp.int32))

    def part(group, ref, first, shards, owner_core, owner_side):
        split, share, across = layout[group]
        index = owner_side * 2 + owner_core if across else owner_core
        start = pl.multiple_of(index * share, share)
        rows = pl.ds(first, shards)
        if split == "columns":
            return ref.at[rows, :, pl.ds(start, share)]
        if split == "rows":
            return ref.at[rows, pl.ds(start, share), :]
        return ref.at[rows]

    slot_y, slot_x, slot_own, slot_far = (2 * z_count + i * z_count for i in range(4))

    def copy(group, source, first, shards, owner_core, owner_side, slot, target):
        return pltpu.make_async_remote_copy(
            src_ref=part(group, source, first, shards, owner_core, owner_side),
            dst_ref=part(group, whole[group], first, shards, owner_core, owner_side),
            send_sem=send_sem.at[group, slot],
            recv_sem=recv_sem.at[group, slot],
            device_id=target,
            device_id_type=MESH,
        )

    def own_part(group):
        return part(group, local[group], 0, 1, core, side)

    def keep_own(group):
        return pltpu.make_async_copy(
            own_part(group), part(group, whole[group], shard, 1, core, side), own_sem.at[group]
        )

    def along(group, origin, distance, up):
        slot = (0 if up else z_count) + distance
        source = whole[group]
        if distance == 0:
            src = own_part(group)
        else:
            src = part(group, source, origin * 2 + y, 1, core, side)
        return pltpu.make_async_remote_copy(
            src_ref=src, dst_ref=part(group, whole[group], origin * 2 + y, 1, core, side),
            send_sem=send_sem.at[group, slot], recv_sem=recv_sem.at[group, slot],
            device_id=(rep, shard + 2 if up else shard - 2), device_id_type=MESH)

    def to_y(group, origin, own):
        if own:
            src = own_part(group)
        else:
            src = part(group, whole[group], origin * 2 + y, 1, core, side)
        return pltpu.make_async_remote_copy(
            src_ref=src, dst_ref=part(group, whole[group], origin * 2 + y, 1, core, side),
            send_sem=send_sem.at[group, slot_y + origin], recv_sem=recv_sem.at[group, slot_y + origin],
            device_id=(rep, peer_y), device_id_type=MESH)

    def from_y(group, origin):
        dst = part(group, whole[group], origin * 2 + 1 - y, 1, core, side)
        return pltpu.make_async_remote_copy(
            src_ref=dst, dst_ref=dst,
            send_sem=send_sem.at[group, slot_y + origin], recv_sem=recv_sem.at[group, slot_y + origin],
            device_id=(rep, peer_y), device_id_type=MESH)

    def to_x(group, origin, mine):
        return copy(group, whole[group], origin * 2, 2, core, side if mine else 1 - side, slot_x + origin, (peer_side, shard))

    def to_core(group, origin, mine_core, mine_side):
        return copy(group, whole[group], origin * 2, 2, core if mine_core else 1 - core, side if mine_side else 1 - side,
                    (slot_own if mine_side else slot_far) + origin, (peer_core, shard))

    steps = [(d, up) for d in range(1, z_count) for up in (True, False)]

    def valid(d, up):
        return z - d >= 0 if up else z + d < z_count

    for group in range(count):
        keep_own(group).start()
    for group in range(count):
        @pl.when(has_up)
        def _(group=group):
            along(group, z, 0, True).start()
        @pl.when(has_down)
        def _(group=group):
            along(group, z, 0, False).start()
        to_y(group, z, True).start()
    for group in range(count):
        keep_own(group).wait()

    def finish_pair(group, origin):
        from_y(group, origin).wait_recv()
        split, share, across = layout[group]
        if across:
            to_x(group, origin, True).start()
        if split is not None:
            to_core(group, origin, True, True).start()

    for group in range(count):
        across = layout[group][2]
        pending = []
        for d, up in steps:
            origin = z - d if up else z + d
            @pl.when(valid(d, up))
            def _(group=group, d=d, up=up, origin=origin):
                along(group, origin, d - 1, up).wait_recv()
                further = has_up if up else has_down
                if d < z_count - 1:
                    @pl.when(further)
                    def _():
                        along(group, origin, d, up).start()
                to_y(group, origin, False).start()
            if d == 1 and not up:
                finish_pair(group, z)
            if d > 1 and not up:
                for u in (True, False):
                    o = z - d + 1 if u else z + d - 1
                    @pl.when(valid(d - 1, u))
                    def _(group=group, o=o):
                        finish_pair(group, o)
        d = z_count - 1
        for u in (True, False):
            o = z - d if u else z + d
            @pl.when(valid(d, u))
            def _(group=group, o=o):
                finish_pair(group, o)

    order = [(0, True)] + steps
    def each(fn):
        for d, up in order:
            o = z - d if up else z + d
            if d == 0:
                fn(o)
            else:
                @pl.when(valid(d, up))
                def _(o=o):
                    fn(o)
    for group in range(count):
        if layout[group][2]:
            def relay(o, group=group):
                to_x(group, o, False).wait_recv()
                to_core(group, o, True, False).start()
            each(relay)
    for group in range(count):
        split, share, across = layout[group]
        def last(o, group=group, split=split, across=across):
            if split is not None:
                to_core(group, o, False, True).wait_recv()
            if across:
                to_core(group, o, False, False).wait_recv()
        each(last)
    for group in range(count):
        split, share, across = layout[group]
        @pl.when(has_up)
        def _(group=group):
            along(group, z, 0, True).wait_send()
        @pl.when(has_down)
        def _(group=group):
            along(group, z, 0, False).wait_send()
        for d, up in steps:
            if d < z_count - 1:
                origin = z - d if up else z + d
                @pl.when(jnp.logical_and(valid(d, up), has_up if up else has_down))
                def _(group=group, d=d, up=up, origin=origin):
                    along(group, origin, d, up).wait_send()
        def sent(o, group=group, split=split, across=across):
            to_y(group, o, False).wait_send()
            if across:
                to_x(group, o, True).wait_send()
                to_core(group, o, True, False).wait_send()
            if split is not None:
                to_core(group, o, True, True).wait_send()
        each(sent)

def gather_all(local, layout, shards, collective_id, cost=0):
    count = len(local)
    z_count = shards // 2
    slots = 6 * z_count
    return pl.pallas_call(
        partial(gather_kernel, layout, z_count),
        out_shape=[jax.ShapeDtypeStruct((shards,) + a.shape, a.dtype) for a in local],
        in_specs=[pl.BlockSpec(memory_space=pltpu.VMEM)] * count,
        out_specs=[pl.BlockSpec(memory_space=pl.ANY)] * count,
        scratch_shapes=[pltpu.SemaphoreType.DMA((count, slots)), pltpu.SemaphoreType.DMA((count, slots)), pltpu.SemaphoreType.DMA((count,))],
        compiler_params=pltpu.CompilerParams(collective_id=collective_id, has_side_effects=True),
        name="gather_weights",
        cost_estimate=pl.CostEstimate(flops=0, bytes_accessed=cost, transcendentals=0),
    )(*[a[None] for a in local])


def swap(value, bit):
    count = lax.axis_size("rep")
    return lax.ppermute(value, "rep", [(i, i ^ bit) for i in range(count)])


def over_groups(value):
    bit = 4
    while bit < lax.axis_size("rep"):
        value = value + swap(value, bit)
        bit *= 2
    return value


def per_device(
    tokens,
    lengths,
    seq_order,
    w_query,
    w_key,
    w_value,
    w_out,
    b_query,
    b_value,
    b_out,
    ln1_gain,
    ln1_bias,
    w_up,
    b_up,
    w_down,
    b_down,
    ln2_gain,
    ln2_bias,
    cotangent,
):
    device_count = lax.axis_size(("rep", "shard"))
    shards = lax.axis_size("shard")
    seq_count, seq_len, model_width = cotangent.shape
    hidden_width = w_up.shape[1]
    part_len = tokens.shape[1]
    score_scale = float(model_width // HEADS) ** (-0.5)
    row_count = seq_count * seq_len
    slot_table = seq_order.reshape(device_count, seq_count).T
    picked = tokens[slot_table]
    arrived = lax.all_to_all(picked, ("rep", "shard"), split_axis=1, concat_axis=1, tiled=True)
    tok_rows = arrived.reshape(row_count, model_width)
    my_index = lax.axis_index(("rep", "shard"))
    my_slots = lax.dynamic_slice_in_dim(seq_order, my_index * seq_count, seq_count)
    my_lengths = lengths[my_slots]
    key_mask = jnp.arange(seq_len, dtype=jnp.int32)[None, :] < my_lengths[:, None]
    valid_rows = key_mask.reshape(row_count, 1).astype(jnp.float32)

    w_attn = jnp.concatenate([w_query, w_key, w_value, w_out], axis=1)
    vectors = (b_query, b_value, b_out, ln1_gain, ln1_bias, b_down, ln2_gain, ln2_bias, b_up)
    packed = jnp.concatenate(vectors)
    room = 16 * PAIR
    packed = jnp.pad(packed, (0, room - packed.shape[0])).reshape(16, PAIR)
    layout = (
        ("columns", model_width, True),
        ("columns", hidden_width // 4, True),
        ("rows", w_down.shape[0] // 2, False),
        (None, 0, False),
    )
    all_attn, all_up, all_down, all_small = gather_all(
        (w_attn, w_up, w_down, packed), layout, shards, collective_id=1, cost=100 << 20
    )
    all_attn = all_attn.reshape(model_width, 4 * model_width)
    all_up = all_up.reshape(model_width, hidden_width)
    all_down = all_down.reshape(hidden_width, model_width)
    flat = all_small.reshape(shards, room).astype(jnp.float32)
    small = []
    at = 0
    for vector in vectors:
        size = vector.shape[0]
        small.append(flat[:, at : at + size].reshape(shards * size))
        at += size
    f_b_query, f_b_value, f_b_out, gain_one, f_ln1_bias, f_b_down, gain_two, f_ln2_bias, f_b_up = small

    w_in = all_attn[:, : 3 * model_width]
    w_out_all = all_attn[:, 3 * model_width :]
    bias_in = jnp.concatenate([f_b_query, jnp.zeros_like(f_b_query), f_b_value])
    projected = (jnp.dot(tok_rows, w_in, preferred_element_type=jnp.float32) + bias_in).astype(jnp.bfloat16)
    context, probs = attend_forward(projected, my_lengths, seq_count, seq_len, model_width, score_scale)
    attn_out = jnp.dot(context, w_out_all, preferred_element_type=jnp.float32) + f_b_out
    resid_one = tok_rows.astype(jnp.float32) + attn_out
    normed_one, inv_one = norm_stats(resid_one)
    hidden_one = normed_one * gain_one + f_ln1_bias
    hidden_low = hidden_one.astype(jnp.bfloat16)
    up_proj = jnp.dot(hidden_low, all_up, preferred_element_type=jnp.float32) + f_b_up
    activated, gelu_pull = jax.vjp(exact_gelu, up_proj)
    act_low = activated.astype(jnp.bfloat16)
    ffn_out = jnp.dot(act_low, all_down, preferred_element_type=jnp.float32) + f_b_down
    resid_two = hidden_one + ffn_out
    normed_two, inv_two = norm_stats(resid_two)
    result_rows = normed_two * gain_two + f_ln2_bias
    outputs = result_rows.astype(jnp.bfloat16).reshape(seq_count, seq_len, model_width)
    grad_out = cotangent.reshape(row_count, model_width).astype(jnp.float32) * valid_rows
    d_ln2_gain = jnp.sum(grad_out * normed_two, axis=0)
    d_ln2_bias = jnp.sum(grad_out, axis=0)
    grad_resid_two = norm_back(grad_out, normed_two, inv_two, gain_two)
    grad_ffn = grad_resid_two.astype(jnp.bfloat16)
    d_w_down = contract_rows(act_low, grad_ffn).astype(jnp.bfloat16)
    d_b_down = jnp.sum(grad_ffn.astype(jnp.float32), axis=0)
    grad_act = contract_cols(grad_ffn, all_down)
    grad_up = gelu_pull(grad_act)[0].astype(jnp.bfloat16)
    d_w_up = contract_rows(hidden_low, grad_up).astype(jnp.bfloat16)
    d_b_up = jnp.sum(grad_up.astype(jnp.float32), axis=0)
    grad_hidden = grad_resid_two + contract_cols(grad_up, all_up)
    d_ln1_gain = jnp.sum(grad_hidden * normed_one, axis=0)
    d_ln1_bias = jnp.sum(grad_hidden, axis=0)
    grad_resid_one = norm_back(grad_hidden, normed_one, inv_one, gain_one)
    grad_attn = grad_resid_one.astype(jnp.bfloat16)
    d_w_out = contract_rows(context, grad_attn).astype(jnp.bfloat16)
    d_b_out = jnp.sum(grad_attn.astype(jnp.float32), axis=0)
    grad_context = contract_cols(grad_attn, w_out_all).astype(jnp.bfloat16)
    grad_projected, up_quarters, down_quarters = attend_backward(
        projected, grad_context, probs, d_w_up, d_w_down, shards, seq_count, seq_len, model_width, score_scale, collective_id=2
    )
    grad_rows = grad_resid_one + contract_cols(grad_projected, w_in)
    back_rows = grad_rows.astype(jnp.bfloat16).reshape(seq_count, device_count, part_len, model_width)
    returned = lax.all_to_all(back_rows, ("rep", "shard"), split_axis=1, concat_axis=1, tiled=True)
    d_w_in = contract_rows(tok_rows, grad_projected).astype(jnp.bfloat16)
    grad_wide = grad_projected.astype(jnp.float32)
    d_b_query = jnp.sum(grad_wide[:, :model_width], axis=0)
    d_b_value = jnp.sum(grad_wide[:, 2 * model_width :], axis=0)
    d_small = (d_b_query, d_b_value, d_b_out, d_ln1_gain, d_ln1_bias, d_b_down, d_ln2_gain, d_ln2_bias, d_b_up)
    rows = jnp.concatenate([d.reshape(shards, -1) for d in d_small], axis=1)
    rows = jnp.pad(rows, ((0, 0), (0, room - rows.shape[1]))).reshape(shards, 16, PAIR)
    attn_quarters, total = reduce_last(jnp.concatenate([d_w_in, d_w_out], axis=1), rows, shards, collective_id=3)
    attn_quarters, total = over_groups(attn_quarters), over_groups(total)
    up_quarters, down_quarters = over_groups(up_quarters), over_groups(down_quarters)
    total = total.reshape(room)
    small_out = []
    at = 0
    for vector in vectors:
        size = vector.shape[0]
        small_out.append(total[at : at + size])
        at += size
    g_b_query, g_b_value, g_b_out, g_ln1_gain, g_ln1_bias, g_b_down, g_ln2_gain, g_ln2_bias, g_b_up = small_out

    every = jnp.arange(seq_order.shape[0], dtype=jnp.int32)
    slot_of = jnp.sum(jnp.where(seq_order[None, :] == every[:, None], every[None, :], 0), axis=1)
    by_slot = returned.transpose(1, 0, 2, 3).reshape(device_count * seq_count, part_len, model_width)
    grad_tokens = by_slot[slot_of]
    g_up = jnp.concatenate([up_quarters[i] for i in range(4)], axis=1).astype(jnp.float32)
    g_down = down_quarters.reshape(w_down.shape).astype(jnp.float32)
    g_attn = [attn_quarters[i].astype(jnp.float32) for i in range(4)]
    return (
        outputs,
        grad_tokens,
        *g_attn,
        g_b_query,
        g_b_value,
        g_b_out,
        g_ln1_gain,
        g_ln1_bias,
        g_up,
        g_b_up,
        g_down,
        g_b_down,
        g_ln2_gain,
        g_ln2_bias,
    )


def solution(mesh):
    in_specs = (
        P(None, ("rep", "shard"), None),
        P(),
        P(),
        P("shard", None),
        P("shard", None),
        P("shard", None),
        P("shard", None),
        P("shard"),
        P("shard"),
        P("shard"),
        P("shard"),
        P("shard"),
        P("shard", None),
        P("shard"),
        P("shard", None),
        P("shard"),
        P("shard"),
        P("shard"),
        P(("rep", "shard"), None, None),
    )
    out_specs = (
        P(("rep", "shard"), None, None),
        P(None, ("rep", "shard"), None),
        P("shard", None),
        P("shard", None),
        P("shard", None),
        P("shard", None),
        P("shard"),
        P("shard"),
        P("shard"),
        P("shard"),
        P("shard"),
        P("shard", None),
        P("shard"),
        P("shard", None),
        P("shard"),
        P("shard"),
        P("shard"),
    )
    return jax.shard_map(
        per_device, mesh=mesh, in_specs=in_specs, out_specs=out_specs, check_vma=False
    )
```

```python
from functools import partial

import jax
import jax.numpy as jnp
from jax import lax
from jax.experimental import pallas as pl
from jax.experimental.pallas import tpu as pltpu
from jax.sharding import PartitionSpec as P

HEADS = 12
HEAD_DIM = 64
PAIR = 128
NEG_FILL = -1e30
EPS_NORM = 1e-12
LOG2E = 1.4426950408889634
MESH = pl.DeviceIdType.MESH


def contract_rows(left, right):
    return lax.dot_general(
        left, right, (((0,), (0,)), ((), ())), preferred_element_type=jnp.float32
    )


def contract_cols(left, right):
    return lax.dot_general(
        left, right, (((1,), (1,)), ((), ())), preferred_element_type=jnp.float32
    )


def norm_stats(resid):
    row_mean = jnp.mean(resid, axis=-1, keepdims=True)
    centered = resid - row_mean
    variance = jnp.mean(centered * centered, axis=-1, keepdims=True)
    inv_std = lax.rsqrt(variance + EPS_NORM)
    return (centered * inv_std, inv_std)


def norm_back(grad_in, normed, inv_std, gain):
    scaled = grad_in * gain
    mean_grad = jnp.mean(scaled, axis=-1, keepdims=True)
    mean_cross = jnp.mean(scaled * normed, axis=-1, keepdims=True)
    return inv_std * (scaled - mean_grad - normed * mean_cross)


class Spot:
    def __init__(self, z_count):
        self.rep, self.shard = lax.axis_index("rep"), lax.axis_index("shard")
        self.z_count = z_count
        self.core, self.side = self.rep % 2, (self.rep // 2) % 2
        self.y, self.z = self.shard % 2, self.shard // 2
        core_step, side_step = 1 - 2 * self.core, 2 - 4 * self.side
        self.over_core = (self.rep + core_step, self.shard)
        self.over_x = (self.rep + side_step, self.shard)
        self.over_y = (self.rep, self.shard + 1 - 2 * self.y)

    def z_after(self, step):
        return lax.rem(self.z + step, self.z_count)

    def ahead(self, step):
        return (self.rep, 2 * self.z_after(step) + self.y)

    def greet(self):
        barrier = pltpu.get_barrier_semaphore()
        targets = [self.over_core, self.over_x, self.over_y]
        targets += [self.ahead(step) for step in range(1, self.z_count)]
        for target in targets:
            pl.semaphore_signal(barrier, inc=1, device_id=target, device_id_type=MESH)
        pl.semaphore_wait(barrier, len(targets))


def sum_slots(z_count):
    return 7 * z_count + 3


def sum_scratch(z_count, rows, columns):
    low = jnp.bfloat16
    return [
        pltpu.VMEM((z_count, 2, 2, rows, columns), low),
        pltpu.VMEM((z_count, 2, 2, rows, columns), low),
        pltpu.VMEM((z_count, 2, rows, columns), low),
        pltpu.VMEM((z_count, rows, columns), low),
        pltpu.VMEM((z_count, rows, columns), low),
        pltpu.VMEM((rows, columns), low),
        pltpu.SemaphoreType.DMA((sum_slots(z_count),)),
        pltpu.SemaphoreType.DMA((sum_slots(z_count),)),
        pltpu.SemaphoreType.DMA((4 * z_count + 1,)),
    ]


class WeightSum:
    def __init__(self, spot, grad, result, pattern, scratch):
        self.spot, self.grad, self.result, self.pattern = spot, grad, result, pattern
        self.own, self.core_in, self.wide_in, self.thin_in, self.line_in, self.total = scratch[:6]
        self.send_sem, self.recv_sem, self.load_sem = scratch[6:]
        self.count = spot.z_count
        self.quarter = 2 * spot.side + spot.core

    def x_first(self, i):
        return self.pattern[i % len(self.pattern)] == "x"

    def block(self, shard, quarter):
        rows, width = self.total.shape
        if len(self.grad.shape) == 2:
            return self.grad.at[pl.ds(pl.multiple_of((4 * shard + quarter) * rows, rows), rows)]
        return self.grad.at[shard, :, pl.ds(pl.multiple_of(quarter * width, width), width)]

    def remote(self, slot, source, target_ref, device):
        return pltpu.make_async_remote_copy(
            src_ref=source, dst_ref=target_ref, send_sem=self.send_sem.at[slot], recv_sem=self.recv_sem.at[slot],
            device_id=device, device_id_type=MESH)

    def place(self, i, s, y):
        spot = self.spot
        shard = 2 * spot.z_after(i + 1) + (spot.y if y else 1 - spot.y)
        return shard, 2 * (spot.side if s else 1 - spot.side)

    def to_core(self, i, s, y):
        shard, base = self.place(i, s, y)
        return self.remote(4 * i + 2 * s + y, self.block(shard, base + 1 - self.spot.core), self.core_in.at[i, s, y], self.spot.over_core)

    def load(self, i, s, y):
        shard, base = self.place(i, s, y)
        return pltpu.make_async_copy(self.block(shard, base + self.spot.core), self.own.at[i, s, y], self.load_sem.at[4 * i + 2 * s + y])

    def wide(self, i):
        source = self.own.at[i, 0] if self.x_first(i) else self.own.at[i, :, 0]
        return self.remote(4 * self.count + i, source, self.wide_in.at[i], self.spot.over_x if self.x_first(i) else self.spot.over_y)

    def thin(self, i):
        source = self.own.at[i, 1, 0] if self.x_first(i) else self.own.at[i, 0, 1]
        return self.remote(5 * self.count + i, source, self.thin_in.at[i], self.spot.over_y if self.x_first(i) else self.spot.over_x)

    def line(self, i):
        return self.remote(6 * self.count + i, self.own.at[i, 1, 1], self.line_in.at[i], self.spot.ahead(i + 1))

    def keep(self):
        return pltpu.make_async_copy(self.total, self.result.at[self.quarter], self.load_sem.at[4 * self.count])

    def spread(self, which, arriving=False):
        spot = self.spot
        far_core, far_side = (arriving and which != 1), (which == 2 or (arriving and which == 1))
        core = 1 - spot.core if far_core else spot.core
        side = 1 - spot.side if far_side else spot.side
        there = self.result.at[2 * side + core]
        source = there if which == 2 else self.total
        return self.remote(7 * self.count + which, source, there, spot.over_x if which == 1 else spot.over_core)

    def begin(self):
        for i in range(self.count):
            for s in range(2):
                for y in range(2):
                    self.to_core(i, s, y).start()
                    self.load(i, s, y).start()

    def add_core(self, i, s, y):
        self.to_core(i, s, y).wait_recv()
        self.load(i, s, y).wait()
        self.own[i, s, y] = self.own[i, s, y] + self.core_in[i, s, y]

    def step_wide(self, i):
        for other in range(2):
            self.add_core(i, *((0, other) if self.x_first(i) else (other, 0)))
        self.wide(i).start()
        for other in range(2):
            self.add_core(i, *((1, other) if self.x_first(i) else (other, 1)))

    def step_thin(self, i):
        self.wide(i).wait_recv()
        for other in range(2):
            at = (1, other) if self.x_first(i) else (other, 1)
            self.own[i, at[0], at[1]] = self.own[i, at[0], at[1]] + self.wide_in[i, other]
            if other == 0:
                self.thin(i).start()

    def step_line(self, i):
        self.thin(i).wait_recv()
        self.own[i, 1, 1] = self.own[i, 1, 1] + self.thin_in[i]
        if i < self.count - 1:
            self.line(i).start()

    def step_total(self):
        total = self.own[self.count - 1, 1, 1].astype(jnp.float32)
        for i in range(self.count - 1):
            self.line(i).wait_recv()
            total = total + self.line_in[i].astype(jnp.float32)
        self.total[...] = total.astype(jnp.bfloat16)
        self.keep().start()
        self.spread(1).start()
        self.spread(0).start()

    def step_relay(self):
        self.spread(1, True).wait_recv()
        self.spread(2).start()

    def end(self):
        self.spread(0, True).wait_recv()
        self.spread(2, True).wait_recv()
        self.keep().wait()
        for i in range(self.count):
            for s in range(2):
                for y in range(2):
                    self.to_core(i, s, y).wait_send()
            self.wide(i).wait_send()
            self.thin(i).wait_send()
            if i < self.count - 1:
                self.line(i).wait_send()
        for which in range(3):
            self.spread(which).wait_send()

    def turns(self):
        listed = [partial(self.step_wide, i) for i in range(self.count)]
        for i in range(self.count):
            listed.append(partial(self.step_thin, i))
            if i > 0:
                listed.append(partial(self.step_line, i - 1))
        return listed + [partial(self.step_line, self.count - 1)]

    def finish(self):
        self.step_total()
        self.step_relay()
        self.end()


class VectorSum:
    def __init__(self, spot, local, result, scratch):
        self.spot, self.local, self.result = spot, local, result
        self.core_in, self.x_in, self.y_in, self.line_in, self.core_sum, self.x_sum, self.y_sum = scratch[:7]
        self.send_sem, self.recv_sem = scratch[7:]

    def remote(self, slot, source, target_ref, device):
        return pltpu.make_async_remote_copy(
            src_ref=source, dst_ref=target_ref, send_sem=self.send_sem.at[slot], recv_sem=self.recv_sem.at[slot],
            device_id=device, device_id_type=MESH)

    def to_core(self):
        return self.remote(0, self.local, self.core_in, self.spot.over_core)

    def to_x(self):
        return self.remote(1, self.core_sum, self.x_in, self.spot.over_x)

    def to_y(self):
        return self.remote(2, self.x_sum.at[:, 1 - self.spot.y], self.y_in, self.spot.over_y)

    def line(self, i):
        return self.remote(3 + i, self.y_sum.at[self.spot.z_after(i + 1)], self.line_in.at[i], self.spot.ahead(i + 1))

    def begin(self):
        self.to_core().start()

    def step_x(self):
        self.to_core().wait_recv()
        self.core_sum[...] = self.local[...] + self.core_in[...]
        self.to_x().start()

    def step_y(self):
        self.to_x().wait_recv()
        self.x_sum[...] = self.core_sum[...] + self.x_in[...]
        self.to_y().start()

    def step_line(self):
        self.to_y().wait_recv()
        self.y_sum[...] = self.x_sum[:, self.spot.y] + self.y_in[...]
        for i in range(self.spot.z_count - 1):
            self.line(i).start()

    def step_total(self):
        total = self.y_sum[self.spot.z]
        for i in range(self.spot.z_count - 1):
            self.line(i).wait_recv()
            total = total + self.line_in[i]
        self.result[...] = total

    def end(self):
        self.to_core().wait_send()
        self.to_x().wait_send()
        self.to_y().wait_send()
        for i in range(self.spot.z_count - 1):
            self.line(i).wait_send()


def vector_scratch(z_count):
    pair, single = (z_count, 2, 16, PAIR), (z_count, 16, PAIR)
    shapes = (pair, pair, single, single, pair, pair, single)
    return [pltpu.VMEM(shape, jnp.float32) for shape in shapes] + [
        pltpu.SemaphoreType.DMA((3 + z_count,)), pltpu.SemaphoreType.DMA((3 + z_count,))]


def reduce_kernel(grad, vectors, result, vector_result, *scratch):
    z_count = vectors.shape[0]
    spot = Spot(z_count)
    spot.greet()
    weight = WeightSum(spot, grad, result, "xy", scratch[:9])
    vector = VectorSum(spot, vectors, vector_result, scratch[9:])
    weight.begin()
    vector.begin()
    for i in range(z_count):
        weight.step_wide(i)
        if i == 0:
            vector.step_x()
        if i == 2:
            vector.step_y()
    for i in range(z_count):
        weight.step_thin(i)
        if i > 0:
            weight.step_line(i - 1)
        if i == 0:
            vector.step_line()
    vector.step_total()
    weight.step_line(z_count - 1)
    weight.step_total()
    weight.step_relay()
    weight.end()
    vector.end()


def reduce_last(grad, vectors, shards, collective_id):
    z_count = shards // 2
    rows, columns = grad.shape[0] // shards, grad.shape[1] // 4
    return pl.pallas_call(
        reduce_kernel,
        out_shape=[jax.ShapeDtypeStruct((4, rows, columns), jnp.bfloat16), jax.ShapeDtypeStruct((16, PAIR), jnp.float32)],
        in_specs=[pl.BlockSpec(memory_space=pl.ANY), pl.BlockSpec(memory_space=pltpu.VMEM)],
        out_specs=[pl.BlockSpec(memory_space=pl.ANY), pl.BlockSpec(memory_space=pltpu.VMEM)],
        scratch_shapes=sum_scratch(z_count, rows, columns) + vector_scratch(z_count),
        compiler_params=pltpu.CompilerParams(collective_id=collective_id, has_side_effects=True),
        name="reduce_last",
        cost_estimate=pl.CostEstimate(flops=0, bytes_accessed=100 << 20, transcendentals=0),
    )(grad.reshape(shards, rows, 4 * columns), vectors.reshape(z_count, 2, 16, PAIR))


class WeightSpread:
    def __init__(self, spot, local, whole, pattern, rows, sems):
        self.spot, self.local, self.whole, self.pattern, self.rows = spot, local, whole, pattern, rows
        self.send_sem, self.recv_sem, self.load_sem = sems
        self.count = spot.z_count
        self.wide_rows = len(whole.shape) == 2

    def span(self, index, size):
        return pl.ds(pl.multiple_of(index * size, size), size)

    def block(self, shard, quarter):
        if self.wide_rows:
            return self.whole.at[self.span(4 * shard + quarter, self.rows)]
        return self.whole.at[shard, :, self.span(quarter, self.whole.shape[2] // 4)]

    def local_block(self):
        quarter = 2 * self.spot.side + self.spot.core
        if self.wide_rows:
            return self.local.at[self.span(quarter, self.rows)]
        return self.local.at[:, self.span(quarter, self.whole.shape[2] // 4)]

    def at(self, i, far, far_core=False):
        spot = self.spot
        far_y, far_side = far
        shard = 2 * spot.z_after(self.count - 1 - i) + (1 - spot.y if far_y else spot.y)
        quarter = 2 * (1 - spot.side if far_side else spot.side) + (1 - spot.core if far_core else spot.core)
        return self.block(shard, quarter)

    def copy(self, slot, source, there, device):
        return pltpu.make_async_remote_copy(
            src_ref=source, dst_ref=there, send_sem=self.send_sem.at[slot], recv_sem=self.recv_sem.at[slot],
            device_id=device, device_id_type=MESH)

    def axes(self, i):
        if self.pattern[i % len(self.pattern)] == "x":
            return ((0, 0), (0, 1), (1, 0), (1, 1)), self.spot.over_x, self.spot.over_y
        return ((0, 0), (1, 0), (0, 1), (1, 1)), self.spot.over_y, self.spot.over_x

    def sent(self, i, which):
        places, first, second = self.axes(i)
        place = places[(0, 0, 1, 0, 1, 2, 3)[which]]
        device = (first, second, second)[which] if which < 3 else self.spot.over_core
        there = self.at(i, place)
        source = self.local_block() if place == (0, 0) and i == self.count - 1 else there
        return self.copy(8 * i + which, source, there, device)

    def arrive(self, i, which):
        places, first, second = self.axes(i)
        place = places[(1, 2, 3, 0, 1, 2, 3)[which]]
        there = self.at(i, place, which > 2)
        self.copy(8 * i + which, there, there, self.spot.over_core).wait_recv()

    def line(self, i):
        return self.copy(8 * i + 7, self.local_block(), self.at(self.count - 1, (0, 0)), self.spot.ahead(i + 1))

    def keep(self):
        return pltpu.make_async_copy(self.local_block(), self.at(self.count - 1, (0, 0)), self.load_sem.at[0])

    def begin(self):
        own = self.count - 1
        for which in (0, 1):
            self.sent(own, which).start()
        for i in range(own):
            self.line(i).start()
        self.sent(own, 3).start()
        self.keep().start()

    def step_first(self, i):
        there = self.at(i, (0, 0))
        self.copy(8 * i + 7, there, there, self.spot.over_core).wait_recv()
        for which in (0, 1, 3):
            self.sent(i, which).start()

    def step_second(self, i):
        self.arrive(i, 0)
        self.sent(i, 2).start()
        self.sent(i, 4).start()

    def step_third(self, i):
        for which in (1, 2):
            self.arrive(i, which)
            self.sent(i, 4 + which).start()

    def end(self):
        self.keep().wait()
        for i in range(self.count):
            for which in range(3, 7):
                self.arrive(i, which)
        for i in range(self.count):
            for which in range(7):
                self.sent(i, which).wait_send()
            if i < self.count - 1:
                self.line(i).wait_send()

    def turns(self):
        own = self.count - 1
        listed = [partial(self.step_second, own)]
        for i in range(own):
            listed.append(partial(self.step_first, i))
            listed.append(partial(self.step_third, own) if i == 1 else None)
            if i > 0:
                listed.append(partial(self.step_second, i - 1))
        listed.append(partial(self.step_second, own - 1))
        listed += [partial(self.step_third, i) for i in range(own)]
        if own < 2:
            listed.append(partial(self.step_third, own))
        return [turn for turn in listed if turn is not None]


def spread_sems(z_count):
    return [pltpu.SemaphoreType.DMA((8 * z_count,)), pltpu.SemaphoreType.DMA((8 * z_count,)), pltpu.SemaphoreType.DMA((1,))]


def take_turns(step, start, last, begin, turns, counts, finish):
    turns = list(turns)
    @pl.when(step == start)
    def _():
        begin()
    for at in range(start + 1, last):
        each = counts[min(at - start - 1, len(counts) - 1)]
        due, turns = turns[:each], turns[each:]
        if due:
            @pl.when(step == at)
            def _(due=due):
                for turn in due:
                    turn()
    @pl.when(step == last)
    def _():
        for turn in turns:
            turn()
        finish()


def attend_forward_kernel(
    len_ref, tok_ref, w_ref, bias_ref, b_out_ref, gain_ref, shift_ref, up_local,
    proj_ref, ctx_ref, probs_ref, normed_ref, inv_ref, low_ref, up_all, *sems, scale, z_count, steps,
):
    spot = Spot(z_count)
    spread = WeightSpread(spot, up_local, up_all, "xy", 0, sems)
    pairs = tok_ref.shape[1] // PAIR
    seq_len, width = tok_ref.shape
    step = pl.program_id(0) * pairs + pl.program_id(1)

    def begin():
        spot.greet()
        spread.begin()

    @pl.when(pl.program_id(1) == 0)
    def _():
        for part in range(3):
            cols = slice(part * width, (part + 1) * width)
            made = jnp.dot(tok_ref[...], w_ref[:, cols], preferred_element_type=jnp.float32) + bias_ref[:, cols]
            proj_ref[:, cols] = made.astype(jnp.bfloat16)

    valid = len_ref[pl.program_id(0)]
    key_pos = lax.broadcasted_iota(jnp.int32, (seq_len, PAIR), 0)
    fill = jnp.where(key_pos < valid, 0.0, NEG_FILL)[:, :1]
    first = lax.broadcasted_iota(jnp.int32, (seq_len, PAIR), 1) < HEAD_DIM
    col = pl.multiple_of(pl.program_id(1) * PAIR, PAIR)
    queries = proj_ref[:, pl.ds(col, PAIR)]
    keys = proj_ref[:, pl.ds(width + col, PAIR)]
    values_t = proj_ref[:, pl.ds(2 * width + col, PAIR)].T
    parts = []
    for head in range(2):
        own = first if head == 0 else jnp.logical_not(first)
        head_keys = jnp.where(own, keys, jnp.zeros_like(keys))
        scores = contract_cols(head_keys, queries)
        scaled = scores * (scale * LOG2E) + fill
        top = jnp.max(scaled, axis=0, keepdims=True)
        raised = jnp.exp2(scaled - top)
        total = jnp.sum(raised, axis=0, keepdims=True)
        probs = (raised * (1.0 / total)).astype(jnp.bfloat16)
        probs_ref[head] = probs
        parts.append(jnp.dot(values_t[head * HEAD_DIM : (head + 1) * HEAD_DIM], probs, preferred_element_type=jnp.float32))
    ctx_ref[:, pl.ds(col, PAIR)] = jnp.concatenate(parts, axis=0).T.astype(jnp.bfloat16)

    @pl.when(pl.program_id(1) == pairs - 1)
    def _():
        attn_out = jnp.dot(ctx_ref[...], w_ref[:, 3 * width :], preferred_element_type=jnp.float32) + b_out_ref[...]
        normed, inv_std = norm_stats(tok_ref[...].astype(jnp.float32) + attn_out)
        normed_ref[...] = normed
        inv_ref[...] = inv_std
        low_ref[...] = (normed * gain_ref[...] + shift_ref[...]).astype(jnp.bfloat16)

    take_turns(step, 0, steps - 1, begin, spread.turns(), (2, 1), spread.end)


def attend_forward(tok_rows, lens, w_attn, bias_in, b_out, gain, shift, w_up, shards, seq_count, seq_len, width, scale, collective_id):
    pairs = width // PAIR
    z_count = shards // 2
    rows, hidden = w_up.shape
    def seq(shape):
        return pl.BlockSpec(shape, lambda s, h, n: (s, 0))
    def full(array):
        return pl.BlockSpec(array.shape, lambda s, h, n: (0, 0))
    total = seq_count * seq_len
    grid_spec = pltpu.PrefetchScalarGridSpec(
        num_scalar_prefetch=1, grid=(seq_count, pairs),
        in_specs=[seq((seq_len, width)), full(w_attn), full(bias_in), full(b_out), full(gain), full(shift),
                  pl.BlockSpec(memory_space=pl.ANY)],
        out_specs=[
            seq((seq_len, 3 * width)), seq((seq_len, width)),
            pl.BlockSpec((2, seq_len, seq_len), lambda s, h, n: (s * pairs + h, 0, 0)),
            seq((seq_len, width)), seq((seq_len, 1)), seq((seq_len, width)),
            pl.BlockSpec(memory_space=pl.ANY),
        ],
        scratch_shapes=spread_sems(z_count))
    return pl.pallas_call(
        partial(attend_forward_kernel, scale=scale, z_count=z_count, steps=seq_count * pairs), grid_spec=grid_spec,
        out_shape=[
            jax.ShapeDtypeStruct((total, 3 * width), jnp.bfloat16),
            jax.ShapeDtypeStruct((total, width), jnp.bfloat16),
            jax.ShapeDtypeStruct((seq_count * 2 * pairs, seq_len, seq_len), jnp.bfloat16),
            jax.ShapeDtypeStruct((total, width), jnp.float32),
            jax.ShapeDtypeStruct((total, 1), jnp.float32),
            jax.ShapeDtypeStruct((total, width), jnp.bfloat16),
            jax.ShapeDtypeStruct((shards, rows, hidden), jnp.bfloat16),
        ],
        compiler_params=pltpu.CompilerParams(
            dimension_semantics=("arbitrary", "arbitrary"), collective_id=collective_id, has_side_effects=True),
        name="attend_forward",
    )(lens, tok_rows, w_attn, bias_in, b_out, gain, shift, w_up)


TILE = 512
ROWS = 256


def feed_forward_kernel(
    low_ref, up_ref, b_up_ref, normed_ref, gain1_ref, shift1_ref, b_down_ref, gain2_ref, shift2_ref, cot_ref, valid_ref, down_local,
    act_ref, slope_ref, out_ref, grad_ref, grad_low_ref, sums_ref, down_all, act_keep, down_whole, *sems, z_count, tiles, steps,
):
    spot = Spot(z_count)
    spread = WeightSpread(spot, down_local, down_whole, "xy", down_local.shape[0] // 4, sems[:3])
    step = pl.program_id(0)
    save = pltpu.make_async_copy(down_whole, down_all, sems[3].at[0])

    def begin():
        spot.greet()
        spread.begin()

    def finish():
        spread.end()
        save.start()
        sums_ref[...] = jnp.zeros_like(sums_ref)

    take_turns(step, 0, tiles, begin, spread.turns(), (2,), finish)

    @pl.when(step < tiles)
    def _():
        for r in range(low_ref.shape[0] // ROWS):
            span = slice(r * ROWS, (r + 1) * ROWS)
            up = jnp.dot(low_ref[span], up_ref[...], preferred_element_type=jnp.float32) + b_up_ref[...]
            cdf = 0.5 * (1.0 + lax.erf(up * 0.7071067811865476))
            density = jnp.exp2(up * up * (-0.5 * LOG2E)) * 0.3989422804014327
            act = (up * cdf).astype(jnp.bfloat16)
            act_ref[span] = act
            act_keep[span, pl.ds(pl.multiple_of(step * TILE, TILE), TILE)] = act
            slope_ref[span] = (cdf + up * density).astype(jnp.bfloat16)

    @pl.when(step >= tiles)
    def _():
        span = pl.ds(pl.multiple_of((step - tiles) * ROWS, ROWS), ROWS)
        total = jnp.dot(act_keep[span], down_whole[...], preferred_element_type=jnp.float32) + b_down_ref[...]
        hidden = normed_ref[...] * gain1_ref[...] + shift1_ref[...]
        normed, inv_std = norm_stats(hidden + total)
        out_ref[...] = (normed * gain2_ref[...] + shift2_ref[...]).astype(jnp.bfloat16)
        grad_out = cot_ref[...].astype(jnp.float32) * valid_ref[...]
        grad = norm_back(grad_out, normed, inv_std, gain2_ref[...])
        grad_low = grad.astype(jnp.bfloat16)
        grad_ref[...] = grad
        grad_low_ref[...] = grad_low
        sums_ref[0:1] += jnp.sum(grad_out * normed, axis=0, keepdims=True)
        sums_ref[1:2] += jnp.sum(grad_out, axis=0, keepdims=True)
        sums_ref[2:3] += jnp.sum(grad_low.astype(jnp.float32), axis=0, keepdims=True)

    @pl.when(step == steps - 1)
    def _():
        save.wait()


def feed_forward(low, w_up, b_up, normed, gain1, shift1, b_down, gain2, shift2, cotangent, valid, w_down, shards, collective_id):
    rows, width = low.shape
    hidden = w_up.shape[1]
    z_count, tiles, blocks = shards // 2, hidden // TILE, rows // ROWS
    def full(array):
        return pl.BlockSpec(array.shape, lambda t: (0, 0))
    def tile(height):
        return pl.BlockSpec((height, TILE), lambda t: (0, jnp.minimum(t, tiles - 1)))
    def block(columns):
        return pl.BlockSpec((ROWS, columns), lambda t: (jnp.maximum(t - tiles, 0), 0))
    anywhere = pl.BlockSpec(memory_space=pl.ANY)
    return pl.pallas_call(
        partial(feed_forward_kernel, z_count=z_count, tiles=tiles, steps=tiles + blocks), grid=(tiles + blocks,),
        in_specs=[full(low), tile(width), tile(1), block(width), full(gain1), full(shift1), full(b_down), full(gain2), full(shift2),
                  block(width), block(1), anywhere],
        out_specs=[tile(rows), tile(rows), block(width), block(width), block(width), pl.BlockSpec((8, width), lambda t: (0, 0)), anywhere],
        out_shape=[
            jax.ShapeDtypeStruct((rows, hidden), jnp.bfloat16),
            jax.ShapeDtypeStruct((rows, hidden), jnp.bfloat16),
            jax.ShapeDtypeStruct((rows, width), jnp.bfloat16),
            jax.ShapeDtypeStruct((rows, width), jnp.float32),
            jax.ShapeDtypeStruct((rows, width), jnp.bfloat16),
            jax.ShapeDtypeStruct((8, width), jnp.float32),
            jax.ShapeDtypeStruct((hidden, width), jnp.bfloat16),
        ],
        scratch_shapes=[pltpu.VMEM((rows, hidden), jnp.bfloat16), pltpu.VMEM((hidden, width), jnp.bfloat16)]
        + spread_sems(z_count) + [pltpu.SemaphoreType.DMA((1,))],
        compiler_params=pltpu.CompilerParams(
            dimension_semantics=("arbitrary",), collective_id=collective_id, has_side_effects=True),
        name="feed_forward",
    )(low, w_up, b_up, normed, gain1, shift1, b_down, gain2, shift2, cotangent, valid, w_down)


def feed_backward_kernel(
    grad_low_ref, act_ref, slope_ref, down_ref, up_ref, low_ref, grad_ref, normed_ref, inv_ref, gain_ref, ctx_ref, w_out_ref,
    up_grad_ref, b_up_ref, resid_ref, attn_ref, ctx_grad_ref, w_out_grad_ref, sums_ref, down_sum,
    down_grad, hidden_grad, attn_keep, low_t, *scratch, z_count, tiles, blocks,
):
    spot = Spot(z_count)
    down = WeightSum(spot, down_grad, down_sum, "yx", scratch)
    step = pl.program_id(0)
    steps = 2 * tiles + blocks + 1

    def begin():
        spot.greet()
        down.begin()

    def finish():
        w_out_grad_ref[...] = contract_rows(ctx_ref[...], attn_keep[...]).astype(jnp.bfloat16)
        down.finish()

    @pl.when(step < tiles)
    def _():
        there = pl.ds(pl.multiple_of(step * TILE, TILE), TILE)
        down_grad[there] = contract_rows(act_ref[...], grad_low_ref[...]).astype(jnp.bfloat16)

    @pl.when(step == 0)
    def _():
        low_t[...] = low_ref[...].T

    @pl.when(jnp.logical_and(step >= tiles, step < 2 * tiles))
    def _():
        grad_act = contract_cols(grad_low_ref[...], down_ref[...])
        grad_up = (grad_act * slope_ref[...].astype(jnp.float32)).astype(jnp.bfloat16)
        b_up_ref[...] = jnp.sum(grad_up.astype(jnp.float32), axis=0, keepdims=True)
        up_grad_ref[...] = jnp.dot(low_t[...], grad_up, preferred_element_type=jnp.float32).astype(jnp.bfloat16)
        back = contract_cols(grad_up, up_ref[...])
        @pl.when(step == tiles)
        def _():
            hidden_grad[...] = back
        @pl.when(step > tiles)
        def _():
            hidden_grad[...] += back

    @pl.when(step == 2 * tiles)
    def _():
        sums_ref[...] = jnp.zeros_like(sums_ref)

    @pl.when(jnp.logical_and(step >= 2 * tiles, step < 2 * tiles + blocks))
    def _():
        span = pl.ds(pl.multiple_of((step - 2 * tiles) * ROWS, ROWS), ROWS)
        grad_hidden = hidden_grad[span] + grad_ref[...]
        normed = normed_ref[...]
        sums_ref[0:1] += jnp.sum(grad_hidden * normed, axis=0, keepdims=True)
        sums_ref[1:2] += jnp.sum(grad_hidden, axis=0, keepdims=True)
        resid = norm_back(grad_hidden, normed, inv_ref[...], gain_ref[...])
        resid_ref[...] = resid
        attn = resid.astype(jnp.bfloat16)
        attn_ref[...] = attn
        attn_keep[span] = attn
        sums_ref[2:3] += jnp.sum(attn.astype(jnp.float32), axis=0, keepdims=True)
        ctx_grad_ref[...] = contract_cols(attn, w_out_ref[...]).astype(jnp.bfloat16)

    take_turns(step, tiles, steps - 1, begin, down.turns(), (0, 1, 1, 1, 2), finish)


def feed_backward(grad_low, act, slope, w_down, w_up, low, grad, normed, inv_std, gain, context, w_attn, shards, collective_id):
    rows, width = low.shape
    hidden = w_up.shape[1]
    z_count, tiles, blocks = shards // 2, hidden // TILE, rows // ROWS
    low_rows = hidden // shards // 4
    def full(array):
        return pl.BlockSpec(array.shape, lambda t: (0, 0))
    def first(t):
        return jnp.minimum(t, tiles - 1)
    def second(t):
        return jnp.clip(t - tiles, 0, tiles - 1)
    def block(columns):
        return pl.BlockSpec((ROWS, columns), lambda t: (jnp.clip(t - 2 * tiles, 0, blocks - 1), 0))
    anywhere = pl.BlockSpec(memory_space=pl.ANY)
    return pl.pallas_call(
        partial(feed_backward_kernel, z_count=z_count, tiles=tiles, blocks=blocks), grid=(2 * tiles + blocks + 1,),
        in_specs=[
            full(grad_low),
            pl.BlockSpec((rows, TILE), lambda t: (0, first(t))),
            pl.BlockSpec((rows, TILE), lambda t: (0, second(t))),
            pl.BlockSpec((TILE, width), lambda t: (second(t), 0)),
            pl.BlockSpec((width, TILE), lambda t: (0, second(t))),
            full(low), block(width), block(width), block(1), full(gain), full(context),
            pl.BlockSpec((width, width), lambda t: (0, 3)),
        ],
        out_specs=[
            pl.BlockSpec((width, TILE), lambda t: (0, second(t))),
            pl.BlockSpec((1, TILE), lambda t: (0, second(t))),
            block(width), block(width), block(width),
            pl.BlockSpec((width, width), lambda t: (0, 0)),
            pl.BlockSpec((8, width), lambda t: (0, 0)),
            anywhere,
        ],
        out_shape=[
            jax.ShapeDtypeStruct((width, hidden), jnp.bfloat16),
            jax.ShapeDtypeStruct((1, hidden), jnp.float32),
            jax.ShapeDtypeStruct((rows, width), jnp.float32),
            jax.ShapeDtypeStruct((rows, width), jnp.bfloat16),
            jax.ShapeDtypeStruct((rows, width), jnp.bfloat16),
            jax.ShapeDtypeStruct((width, width), jnp.bfloat16),
            jax.ShapeDtypeStruct((8, width), jnp.float32),
            jax.ShapeDtypeStruct((4, low_rows, width), jnp.bfloat16),
        ],
        scratch_shapes=[
            pltpu.VMEM((hidden, width), jnp.bfloat16), pltpu.VMEM((rows, width), jnp.float32), pltpu.VMEM((rows, width), jnp.bfloat16),
            pltpu.VMEM((width, rows), jnp.bfloat16),
        ] + sum_scratch(z_count, low_rows, width),
        compiler_params=pltpu.CompilerParams(
            dimension_semantics=("arbitrary",), collective_id=collective_id, has_side_effects=True),
        name="feed_backward",
    )(grad_low, act, slope, w_down, w_up, low, grad, normed, inv_std, gain, context, w_attn)


def attend_backward_kernel(q_ref, k_ref, v_ref, gctx_ref, probs_ref, up_ref, out_ref, b_query_ref, b_value_ref, up_sum, *scratch, scale, z_count, steps):
    spot = Spot(z_count)
    up = WeightSum(spot, up_ref, up_sum, "xy", scratch)
    pairs = out_ref.shape[1] // 3 // PAIR
    step = pl.program_id(0) * pairs + pl.program_id(1)

    def begin():
        spot.greet()
        up.begin()

    seq_len = q_ref.shape[0]
    width = out_ref.shape[1] // 3
    first = lax.broadcasted_iota(jnp.int32, (seq_len, PAIR), 1) < HEAD_DIM
    queries = q_ref[...]
    keys_t = k_ref[...].T
    values = v_ref[...]
    grad_ctx = gctx_ref[...]
    gq_parts, gk_parts, gv_parts = [], [], []
    for head in range(2):
        own = first if head == 0 else jnp.logical_not(first)
        head_values = jnp.where(own, values, jnp.zeros_like(values))
        probs_low = probs_ref[head]
        probs = probs_low.astype(jnp.float32)
        grad_probs = lax.dot_general(head_values, grad_ctx, (((1,), (1,)), ((), ())), preferred_element_type=jnp.float32)
        row_dot = jnp.sum(probs * grad_probs, axis=0, keepdims=True)
        grad_scores = (probs * (grad_probs - row_dot)).astype(jnp.bfloat16)
        gv_parts.append(jnp.dot(probs_low, grad_ctx, preferred_element_type=jnp.float32))
        gk_parts.append(jnp.dot(grad_scores, queries, preferred_element_type=jnp.float32))
        gq_parts.append(jnp.dot(keys_t[head * HEAD_DIM : (head + 1) * HEAD_DIM], grad_scores, preferred_element_type=jnp.float32))
    col = pl.multiple_of(pl.program_id(1) * PAIR, PAIR)
    grad_query = (jnp.concatenate(gq_parts, axis=0).T * scale).astype(jnp.bfloat16)
    grad_value = jnp.where(first, gv_parts[0], gv_parts[1]).astype(jnp.bfloat16)
    out_ref[:, pl.ds(col, PAIR)] = grad_query
    out_ref[:, pl.ds(width + col, PAIR)] = (jnp.where(first, gk_parts[0], gk_parts[1]) * scale).astype(jnp.bfloat16)
    out_ref[:, pl.ds(2 * width + col, PAIR)] = grad_value

    @pl.when(step == 0)
    def _():
        b_query_ref[...] = jnp.zeros_like(b_query_ref)
        b_value_ref[...] = jnp.zeros_like(b_value_ref)
    b_query_ref[:, pl.ds(col, PAIR)] += jnp.sum(grad_query.astype(jnp.float32), axis=0, keepdims=True)
    b_value_ref[:, pl.ds(col, PAIR)] += jnp.sum(grad_value.astype(jnp.float32), axis=0, keepdims=True)

    take_turns(step, 0, steps - 1, begin, up.turns(), (0, 0, 1), up.finish)


def attend_backward(projected, grad_context, probs, grad_up, shards, seq_count, seq_len, width, scale, collective_id):
    pairs = width // PAIR
    z_count = shards // 2
    rows, columns = grad_up.shape[0] // shards, grad_up.shape[1] // 4
    anywhere = pl.BlockSpec(memory_space=pl.ANY)
    bias = pl.BlockSpec((1, width), lambda s, h: (0, 0))
    return pl.pallas_call(
        partial(attend_backward_kernel, scale=scale, z_count=z_count, steps=seq_count * pairs), grid=(seq_count, pairs),
        in_specs=[
            pl.BlockSpec((seq_len, PAIR), lambda s, h: (s, h)),
            pl.BlockSpec((seq_len, PAIR), lambda s, h: (s, pairs + h)),
            pl.BlockSpec((seq_len, PAIR), lambda s, h: (s, 2 * pairs + h)),
            pl.BlockSpec((seq_len, PAIR), lambda s, h: (s, h)),
            pl.BlockSpec((2, seq_len, seq_len), lambda s, h: (s * pairs + h, 0, 0)),
            anywhere,
        ],
        out_specs=[pl.BlockSpec((seq_len, 3 * width), lambda s, h: (s, 0)), bias, bias, anywhere],
        out_shape=[
            jax.ShapeDtypeStruct((seq_count * seq_len, 3 * width), jnp.bfloat16),
            jax.ShapeDtypeStruct((1, width), jnp.float32),
            jax.ShapeDtypeStruct((1, width), jnp.float32),
            jax.ShapeDtypeStruct((4, rows, columns), jnp.bfloat16),
        ],
        scratch_shapes=sum_scratch(z_count, rows, columns),
        compiler_params=pltpu.CompilerParams(
            dimension_semantics=("arbitrary", "arbitrary"), collective_id=collective_id, has_side_effects=True),
        name="attend_backward",
        cost_estimate=pl.CostEstimate(flops=0, bytes_accessed=60 << 20, transcendentals=0),
    )(projected, projected, projected, grad_context, probs, grad_up.reshape(shards, rows, 4 * columns))


def gather_kernel(layout, z_count, *refs):
    count = len(layout)
    local = refs[:count]
    whole = refs[count : 2 * count]
    send_sem, recv_sem, own_sem = refs[2 * count :]
    rep = lax.axis_index("rep")
    shard = lax.axis_index("shard")
    z, y = shard // 2, shard % 2
    core = rep % 2
    side = (rep // 2) % 2
    peer_core = rep + 1 - 2 * core
    peer_side = rep + 2 - 4 * side
    peer_y = shard + 1 - 2 * y
    has_up, has_down = z + 1 < z_count, z > 0

    barrier = pltpu.get_barrier_semaphore()
    def greet(target, amount=1):
        pl.semaphore_signal(barrier, inc=amount, device_id=target, device_id_type=MESH)
    greet((peer_core, shard))
    greet((peer_side, shard))
    greet((rep, peer_y))
    @pl.when(has_up)
    def _():
        greet((rep, shard + 2))
    @pl.when(has_down)
    def _():
        greet((rep, shard - 2))
    pl.semaphore_wait(barrier, 3 + has_up.astype(jnp.int32) + has_down.astype(jnp.int32))

    def part(group, ref, first, shards, owner_core, owner_side):
        split, share, across = layout[group]
        index = owner_side * 2 + owner_core if across else owner_core
        start = pl.multiple_of(index * share, share)
        rows = pl.ds(first, shards)
        if split == "columns":
            return ref.at[rows, :, pl.ds(start, share)]
        if split == "rows":
            return ref.at[rows, pl.ds(start, share), :]
        return ref.at[rows]

    slot_y, slot_x, slot_own, slot_far = (2 * z_count + i * z_count for i in range(4))

    def copy(group, source, first, shards, owner_core, owner_side, slot, target):
        return pltpu.make_async_remote_copy(
            src_ref=part(group, source, first, shards, owner_core, owner_side),
            dst_ref=part(group, whole[group], first, shards, owner_core, owner_side),
            send_sem=send_sem.at[group, slot],
            recv_sem=recv_sem.at[group, slot],
            device_id=target,
            device_id_type=MESH,
        )

    def own_part(group):
        return part(group, local[group], 0, 1, core, side)

    def keep_own(group):
        return pltpu.make_async_copy(
            own_part(group), part(group, whole[group], shard, 1, core, side), own_sem.at[group]
        )

    def along(group, origin, distance, up):
        slot = (0 if up else z_count) + distance
        source = whole[group]
        if distance == 0:
            src = own_part(group)
        else:
            src = part(group, source, origin * 2 + y, 1, core, side)
        return pltpu.make_async_remote_copy(
            src_ref=src, dst_ref=part(group, whole[group], origin * 2 + y, 1, core, side),
            send_sem=send_sem.at[group, slot], recv_sem=recv_sem.at[group, slot],
            device_id=(rep, shard + 2 if up else shard - 2), device_id_type=MESH)

    def to_y(group, origin, own):
        if own:
            src = own_part(group)
        else:
            src = part(group, whole[group], origin * 2 + y, 1, core, side)
        return pltpu.make_async_remote_copy(
            src_ref=src, dst_ref=part(group, whole[group], origin * 2 + y, 1, core, side),
            send_sem=send_sem.at[group, slot_y + origin], recv_sem=recv_sem.at[group, slot_y + origin],
            device_id=(rep, peer_y), device_id_type=MESH)

    def from_y(group, origin):
        dst = part(group, whole[group], origin * 2 + 1 - y, 1, core, side)
        return pltpu.make_async_remote_copy(
            src_ref=dst, dst_ref=dst,
            send_sem=send_sem.at[group, slot_y + origin], recv_sem=recv_sem.at[group, slot_y + origin],
            device_id=(rep, peer_y), device_id_type=MESH)

    def to_x(group, origin, mine):
        return copy(group, whole[group], origin * 2, 2, core, side if mine else 1 - side, slot_x + origin, (peer_side, shard))

    def to_core(group, origin, mine_core, mine_side):
        return copy(group, whole[group], origin * 2, 2, core if mine_core else 1 - core, side if mine_side else 1 - side,
                    (slot_own if mine_side else slot_far) + origin, (peer_core, shard))

    steps = [(d, up) for d in range(1, z_count) for up in (True, False)]

    def valid(d, up):
        return z - d >= 0 if up else z + d < z_count

    for group in range(count):
        keep_own(group).start()
    for group in range(count):
        @pl.when(has_up)
        def _(group=group):
            along(group, z, 0, True).start()
        @pl.when(has_down)
        def _(group=group):
            along(group, z, 0, False).start()
        to_y(group, z, True).start()
    for group in range(count):
        keep_own(group).wait()

    def finish_pair(group, origin):
        from_y(group, origin).wait_recv()
        split, share, across = layout[group]
        if across:
            to_x(group, origin, True).start()
        if split is not None:
            to_core(group, origin, True, True).start()

    for group in range(count):
        across = layout[group][2]
        pending = []
        for d, up in steps:
            origin = z - d if up else z + d
            @pl.when(valid(d, up))
            def _(group=group, d=d, up=up, origin=origin):
                along(group, origin, d - 1, up).wait_recv()
                further = has_up if up else has_down
                if d < z_count - 1:
                    @pl.when(further)
                    def _():
                        along(group, origin, d, up).start()
                to_y(group, origin, False).start()
            if d == 1 and not up:
                finish_pair(group, z)
            if d > 1 and not up:
                for u in (True, False):
                    o = z - d + 1 if u else z + d - 1
                    @pl.when(valid(d - 1, u))
                    def _(group=group, o=o):
                        finish_pair(group, o)
        d = z_count - 1
        for u in (True, False):
            o = z - d if u else z + d
            @pl.when(valid(d, u))
            def _(group=group, o=o):
                finish_pair(group, o)

    order = [(0, True)] + steps
    def each(fn):
        for d, up in order:
            o = z - d if up else z + d
            if d == 0:
                fn(o)
            else:
                @pl.when(valid(d, up))
                def _(o=o):
                    fn(o)
    for group in range(count):
        if layout[group][2]:
            def relay(o, group=group):
                to_x(group, o, False).wait_recv()
                to_core(group, o, True, False).start()
            each(relay)
    for group in range(count):
        split, share, across = layout[group]
        def last(o, group=group, split=split, across=across):
            if split is not None:
                to_core(group, o, False, True).wait_recv()
            if across:
                to_core(group, o, False, False).wait_recv()
        each(last)
    for group in range(count):
        split, share, across = layout[group]
        @pl.when(has_up)
        def _(group=group):
            along(group, z, 0, True).wait_send()
        @pl.when(has_down)
        def _(group=group):
            along(group, z, 0, False).wait_send()
        for d, up in steps:
            if d < z_count - 1:
                origin = z - d if up else z + d
                @pl.when(jnp.logical_and(valid(d, up), has_up if up else has_down))
                def _(group=group, d=d, up=up, origin=origin):
                    along(group, origin, d, up).wait_send()
        def sent(o, group=group, split=split, across=across):
            to_y(group, o, False).wait_send()
            if across:
                to_x(group, o, True).wait_send()
                to_core(group, o, True, False).wait_send()
            if split is not None:
                to_core(group, o, True, True).wait_send()
        each(sent)

def gather_all(local, layout, shards, collective_id, cost=0):
    count = len(local)
    z_count = shards // 2
    slots = 6 * z_count
    return pl.pallas_call(
        partial(gather_kernel, layout, z_count),
        out_shape=[jax.ShapeDtypeStruct((shards,) + a.shape, a.dtype) for a in local],
        in_specs=[pl.BlockSpec(memory_space=pltpu.VMEM)] * count,
        out_specs=[pl.BlockSpec(memory_space=pl.ANY)] * count,
        scratch_shapes=[pltpu.SemaphoreType.DMA((count, slots)), pltpu.SemaphoreType.DMA((count, slots)), pltpu.SemaphoreType.DMA((count,))],
        compiler_params=pltpu.CompilerParams(collective_id=collective_id, has_side_effects=True),
        name="gather_weights",
        cost_estimate=pl.CostEstimate(flops=0, bytes_accessed=cost, transcendentals=0),
    )(*[a[None] for a in local])


def swap(value, bit):
    count = lax.axis_size("rep")
    return lax.ppermute(value, "rep", [(i, i ^ bit) for i in range(count)])


def over_groups(value):
    bit = 4
    while bit < lax.axis_size("rep"):
        value = value + swap(value, bit)
        bit *= 2
    return value


def per_device(
    tokens,
    lengths,
    seq_order,
    w_query,
    w_key,
    w_value,
    w_out,
    b_query,
    b_value,
    b_out,
    ln1_gain,
    ln1_bias,
    w_up,
    b_up,
    w_down,
    b_down,
    ln2_gain,
    ln2_bias,
    cotangent,
):
    device_count = lax.axis_size(("rep", "shard"))
    shards = lax.axis_size("shard")
    seq_count, seq_len, model_width = cotangent.shape
    hidden_width = w_up.shape[1]
    part_len = tokens.shape[1]
    score_scale = float(model_width // HEADS) ** (-0.5)
    row_count = seq_count * seq_len
    slot_table = seq_order.reshape(device_count, seq_count).T
    picked = tokens[slot_table]
    arrived = lax.all_to_all(picked, ("rep", "shard"), split_axis=1, concat_axis=1, tiled=True)
    tok_rows = arrived.reshape(row_count, model_width)
    my_index = lax.axis_index(("rep", "shard"))
    my_slots = lax.dynamic_slice_in_dim(seq_order, my_index * seq_count, seq_count)
    my_lengths = lengths[my_slots]
    key_mask = jnp.arange(seq_len, dtype=jnp.int32)[None, :] < my_lengths[:, None]
    valid_rows = key_mask.reshape(row_count, 1).astype(jnp.float32)

    w_attn = jnp.concatenate([w_query, w_key, w_value, w_out], axis=1)
    vectors = (b_query, b_value, b_out, ln1_gain, ln1_bias, b_down, ln2_gain, ln2_bias, b_up)
    packed = jnp.concatenate(vectors)
    room = 16 * PAIR
    packed = jnp.pad(packed, (0, room - packed.shape[0])).reshape(16, PAIR)
    layout = (("columns", model_width, True), (None, 0, False))
    w_attn_all, all_small = gather_all((w_attn, packed), layout, shards, collective_id=1, cost=60 << 20)
    w_attn_all = w_attn_all.reshape(model_width, 4 * model_width)
    flat = all_small.reshape(shards, room).astype(jnp.float32)
    small = []
    at = 0
    for vector in vectors:
        size = vector.shape[0]
        small.append(flat[:, at : at + size].reshape(shards * size))
        at += size
    f_b_query, f_b_value, f_b_out, gain_one, f_ln1_bias, f_b_down, gain_two, f_ln2_bias, f_b_up = small

    bias_in = jnp.concatenate([f_b_query, jnp.zeros_like(f_b_query), f_b_value])[None]
    gain_one, gain_two = gain_one[None], gain_two[None]
    projected, context, probs, normed_one, inv_one, hidden_low, all_up = attend_forward(
        tok_rows, my_lengths, w_attn_all, bias_in, f_b_out[None], gain_one, f_ln1_bias[None], w_up,
        shards, seq_count, seq_len, model_width, score_scale, collective_id=2,
    )
    all_up = all_up.reshape(model_width, hidden_width)
    act_low, slope, out_rows, grad_resid_two, grad_ffn, sums_two, all_down = feed_forward(
        hidden_low, all_up, f_b_up[None], normed_one, gain_one, f_ln1_bias[None], f_b_down[None], gain_two, f_ln2_bias[None],
        cotangent.reshape(row_count, model_width), valid_rows, w_down, shards, collective_id=3,
    )
    outputs = out_rows.reshape(seq_count, seq_len, model_width)
    d_w_up, d_b_up, grad_resid_one, grad_attn, grad_context, d_w_out, sums_one, down_quarters = feed_backward(
        grad_ffn, act_low, slope, all_down, all_up, hidden_low, grad_resid_two, normed_one, inv_one, gain_one, context, w_attn_all,
        shards, collective_id=4,
    )
    d_ln2_gain, d_ln2_bias, d_b_down = sums_two[0], sums_two[1], sums_two[2]
    d_ln1_gain, d_ln1_bias, d_b_out = sums_one[0], sums_one[1], sums_one[2]
    grad_projected, d_b_query, d_b_value, up_quarters = attend_backward(
        projected, grad_context, probs, d_w_up, shards, seq_count, seq_len, model_width, score_scale, collective_id=5
    )
    grad_rows = grad_resid_one + contract_cols(grad_projected, w_attn_all[:, : 3 * model_width])
    back_rows = grad_rows.astype(jnp.bfloat16).reshape(seq_count, device_count, part_len, model_width)
    returned = lax.all_to_all(back_rows, ("rep", "shard"), split_axis=1, concat_axis=1, tiled=True)
    d_w_in = contract_rows(tok_rows, grad_projected).astype(jnp.bfloat16)
    d_small = (d_b_query, d_b_value, d_b_out, d_ln1_gain, d_ln1_bias, d_b_down, d_ln2_gain, d_ln2_bias, d_b_up)
    rows = jnp.concatenate([d.reshape(shards, -1) for d in d_small], axis=1)
    rows = jnp.pad(rows, ((0, 0), (0, room - rows.shape[1]))).reshape(shards, 16, PAIR)
    attn_quarters, total = reduce_last(jnp.concatenate([d_w_in, d_w_out], axis=1), rows, shards, collective_id=6)
    attn_quarters, total = over_groups(attn_quarters), over_groups(total)
    up_quarters, down_quarters = over_groups(up_quarters), over_groups(down_quarters)
    total = total.reshape(room)
    small_out = []
    at = 0
    for vector in vectors:
        size = vector.shape[0]
        small_out.append(total[at : at + size])
        at += size
    g_b_query, g_b_value, g_b_out, g_ln1_gain, g_ln1_bias, g_b_down, g_ln2_gain, g_ln2_bias, g_b_up = small_out

    every = jnp.arange(seq_order.shape[0], dtype=jnp.int32)
    slot_of = jnp.sum(jnp.where(seq_order[None, :] == every[:, None], every[None, :], 0), axis=1)
    by_slot = returned.transpose(1, 0, 2, 3).reshape(device_count * seq_count, part_len, model_width)
    grad_tokens = by_slot[slot_of]
    g_up = jnp.concatenate([up_quarters[i] for i in range(4)], axis=1).astype(jnp.float32)
    g_down = down_quarters.reshape(w_down.shape).astype(jnp.float32)
    g_attn = [attn_quarters[i].astype(jnp.float32) for i in range(4)]
    return (
        outputs,
        grad_tokens,
        *g_attn,
        g_b_query,
        g_b_value,
        g_b_out,
        g_ln1_gain,
        g_ln1_bias,
        g_up,
        g_b_up,
        g_down,
        g_b_down,
        g_ln2_gain,
        g_ln2_bias,
    )


def solution(mesh):
    in_specs = (
        P(None, ("rep", "shard"), None),
        P(),
        P(),
        P("shard", None),
        P("shard", None),
        P("shard", None),
        P("shard", None),
        P("shard"),
        P("shard"),
        P("shard"),
        P("shard"),
        P("shard"),
        P("shard", None),
        P("shard"),
        P("shard", None),
        P("shard"),
        P("shard"),
        P("shard"),
        P(("rep", "shard"), None, None),
    )
    out_specs = (
        P(("rep", "shard"), None, None),
        P(None, ("rep", "shard"), None),
        P("shard", None),
        P("shard", None),
        P("shard", None),
        P("shard", None),
        P("shard"),
        P("shard"),
        P("shard"),
        P("shard"),
        P("shard"),
        P("shard", None),
        P("shard"),
        P("shard", None),
        P("shard"),
        P("shard"),
        P("shard"),
    )
    return jax.shard_map(
        per_device, mesh=mesh, in_specs=in_specs, out_specs=out_specs, check_vma=False
    )
```
